32 devices in a mesh: parts: 2 (over y), freq: 8 (over z, x), seg: 2 (over core).
Axes of the slice: x: 2, y: 2, z: 4, core: 2. Of those that a mesh axis runs over, the one named last changes fastest.
Arguments:
- samples: float32 [8, 2, 1024, 1024], P(('parts', 'seg'), None, 'freq'), parts along dimension 0, may hold values from -6 to 6
- kernels: bfloat16 [2, 8, 128], replicated, may hold values from -0.375 to 0.375
- offsets: int32 [8, 8], P(('parts', 'seg')), parts along dimension 0, may hold values from -4096 to 4096, as said below
- weight_index: int32 [8], P(('parts', 'seg')), parts along dimension 0, may hold values from 0 to 15
- level_weights: float32 [16], replicated, may hold values from 0.1 to 1
Outputs:
- planes: float32 [16, 1048576], P(('parts', 'seg'), 'freq'), parts along dimension 0
The draws below stay inside these ranges and needn't reach their ends.
There are 2 independent parts, one for each index of `parts`. The reference program is written for one: setup_inputs(seed, part) draws one part's arguments, and reference() takes and returns one part's arrays. A program takes and returns all parts, laid end to end along the dimension named above; an argument that names none is the same for every part. Nothing has to cross between parts.
Inputs may be any that keep to these rules, and one draw needn't show every extreme that they name: `offsets`: each offset lies within 4096 blocks of zero; both ends are taken in every draw. Among the 16 offsets of one index of seg, at most 4 have the same quotient by 1024 (rounded down), and in every draw some quotient has exactly 4.
All inputs are finite; a program needn't handle non-finite values.
Results may differ from the reference program's by a relative error of at most 0.01.
Values may be sent and summed in bfloat16 or wider, within the bound.
No kernel may reach another device: no remote copies, remote signals or barrier semaphores. Data moves between devices by JAX's collectives and lax.ppermute only.
A program may use at most 128 MiB of HBM per device.

```python
import math
import jax
import jax.numpy as jnp
from jax import lax

N1 = 1024
N2 = 1024
BLOCK = 128
KERNELS = 8
REACH = 4
LEVELS = 16
SEG_DEV = 2
SEGMENTS = 4
BLOCKS_DEV = 1024
ROUTE_CAP = 4


def offsets_group(group_key):
    planes_one = SEG_DEV * KERNELS
    spread = 2 * REACH + 1
    slots = spread * ROUTE_CAP
    centre = jax.random.randint(jax.random.fold_in(group_key, 1), (), -REACH + 1, REACH)
    slot_dist = jnp.repeat(jnp.arange(spread, dtype=jnp.int32) - REACH, ROUTE_CAP)
    slot_rank = jnp.tile(jnp.arange(ROUTE_CAP, dtype=jnp.int32), spread)
    noise = jax.random.permutation(jax.random.fold_in(group_key, 2), slots).astype(jnp.int32)
    extreme = ((slot_dist == REACH) | (slot_dist == -REACH)) & (slot_rank == 0)
    priority = jnp.where(slot_dist == centre, 0, jnp.where(extreme, 1, 2)).astype(jnp.int32)
    order = jnp.argsort(priority * slots + noise, stable=True)
    chosen = slot_dist[order[:planes_one]]
    placing = jax.random.permutation(jax.random.fold_in(group_key, 3), planes_one)
    quotient = jnp.zeros((planes_one,), jnp.int32).at[placing].set(chosen)
    remainder = jax.random.randint(jax.random.fold_in(group_key, 4), (planes_one,), 0, BLOCKS_DEV)
    remainder = jnp.where(jnp.abs(quotient) == REACH, 0, remainder)
    return (quotient * BLOCKS_DEV + remainder).astype(jnp.int32)


def draw_offsets(key, part):
    groups = SEGMENTS // SEG_DEV
    keys = jax.vmap(lambda number: jax.random.fold_in(key, number))(jnp.arange(groups, dtype=jnp.int32) + 11)
    values = jax.vmap(offsets_group)(keys)
    return values.reshape(SEGMENTS, KERNELS).astype(jnp.int32)


def plant(drawn, stream_key, least, top_value):
    index_at = [jax.random.randint(jax.random.fold_in(stream_key, axis), (), 0, length) for axis, length in enumerate(drawn.shape)]
    main_axis = drawn.shape.index(max(drawn.shape))
    neighbour = index_at[:main_axis] + [(index_at[main_axis] + 1) % drawn.shape[main_axis]] + index_at[main_axis + 1:]
    return drawn.at[tuple(index_at)].set(least).at[tuple(neighbour)].set(top_value)


def block_scale(own_key, extent, pieces, low, largest):
    def one(axis_at, shards_of):
        draws = jax.random.uniform(jax.random.fold_in(jax.random.fold_in(own_key, 6), axis_at), (shards_of,), jnp.float32, low / len(pieces), largest / len(pieces))
        return jnp.repeat(jnp.exp(draws), extent[axis_at] // shards_of).reshape((-1,) + (1,) * (len(extent) - axis_at - 1))

    factor_of = one(*pieces[0])
    for cut in pieces[1:]:
        factor_of = factor_of * one(*cut)
    return factor_of


def bell_draw(own_key, extent, width, bound, shards=(), kind=jnp.bfloat16):
    drawn = jax.random.normal(own_key, extent, jnp.float32) * width
    if len(shards) > 0:
        drawn = block_scale(own_key, extent, shards, -0.22, 0.18) * drawn
    return jnp.clip(drawn, min=-bound, max=bound).astype(kind)


def setup_inputs(seed: int = 0, part: int = 0) -> dict:
    streams_of = jax.random.split(jax.random.key(seed), 6)
    own_keys = jax.random.split(jax.random.fold_in(streams_of[5], part), 6)
    samples = bell_draw(own_keys[0], (SEGMENTS, 2, N1, N2), 1.0, 6.0, ((0, 2), (2, 8)), jnp.float32)
    kernels = bell_draw(streams_of[1], (2, KERNELS, BLOCK), (2 * BLOCK) ** -0.5, 0.375)
    offsets = draw_offsets(jax.random.fold_in(jax.random.fold_in(streams_of[5], part), 71), part)
    weight_index = plant(jax.random.randint(own_keys[3], (SEGMENTS,), 0, LEVELS), jax.random.fold_in(own_keys[3], 1), 0, LEVELS - 1).astype(jnp.int32)
    level_weights = jnp.clip(jnp.exp(jax.random.uniform(streams_of[4], (LEVELS,), jnp.float32, math.log(0.1), math.log(1.0))), 0.1, 1.0)
    return dict(samples=samples, kernels=kernels, offsets=offsets, weight_index=weight_index, level_weights=level_weights)


def reference(samples, kernels, offsets, weight_index, level_weights):
    length = N1 * N2
    half = BLOCK // 2
    places = (half - jnp.arange(BLOCK, dtype=jnp.int32)) % length
    kernel_real = kernels[0].astype(jnp.float32)
    kernel_imag = kernels[1].astype(jnp.float32)
    kernel_full = kernel_real + 1j * kernel_imag
    padded = jnp.zeros((KERNELS, length), kernel_full.dtype).at[:, places].set(kernel_full)
    kernel_freq = jnp.fft.fft(padded, axis=-1)
    weights = level_weights[weight_index]

    def roll_blocks(blocks, shift):
        return jnp.roll(blocks, -shift, axis=0)

    def one_segment(total, inputs):
        segment, shifts, weight = inputs
        series = jnp.transpose(segment[0]).reshape(-1) + 1j * jnp.transpose(segment[1]).reshape(-1)
        spectrum = jnp.fft.fft(series) / math.sqrt(length)
        real_part = lax.optimization_barrier(jnp.real(spectrum).astype(jnp.bfloat16)).astype(jnp.float32)
        imag_part = lax.optimization_barrier(jnp.imag(spectrum).astype(jnp.bfloat16)).astype(jnp.float32)
        rounded = real_part + 1j * imag_part
        filtered = jnp.fft.ifft(jnp.fft.fft(rounded)[None, :] * kernel_freq, axis=-1)
        power = jnp.real(filtered) ** 2 + jnp.imag(filtered) ** 2
        power = lax.optimization_barrier(power.astype(jnp.bfloat16)).astype(jnp.float32)
        blocks = power.reshape(KERNELS, length // BLOCK, BLOCK)
        moved = jax.vmap(roll_blocks)(blocks, shifts)
        return (total + weight * moved, None)
    start = jnp.zeros((KERNELS, length // BLOCK, BLOCK), jnp.float32)
    total, unused = lax.scan(one_segment, start, (samples, offsets, weights))
    return (total / SEGMENTS).reshape(KERNELS, length)
```

```python
import functools
import math

import jax
import jax.numpy as jnp
import numpy as np
from jax import lax
from jax.experimental import pallas as pl
from jax.experimental.pallas import tpu as pltpu
from jax.sharding import PartitionSpec as P

BLOCK = 128
KERNELS = 8
REACH = 4
ROUTE_CAP = 4
CHUNKS = 4


def extended(cells, sides, width):
    for axis, dim in sides:
        count = lax.axis_size(axis)
        head = lax.slice_in_dim(cells, 0, width, axis=dim)
        tail = lax.slice_in_dim(cells, cells.shape[dim] - width, cells.shape[dim], axis=dim)
        cells = jnp.concatenate(
            [
                lax.ppermute(tail, axis, [(i, (i + 1) % count) for i in range(count)]),
                cells,
                lax.ppermute(head, axis, [((i + 1) % count, i) for i in range(count)]),
            ],
            axis=dim,
        )
    return cells


def passed_along(block, axis, distance):
    devices = range(lax.axis_size(axis))
    route = [((i - distance) % len(devices), i) for i in devices]
    return lax.ppermute(block, axis, route)


def dft_table(size):
    rows = lax.broadcasted_iota(jnp.int32, (size, size), 0)
    cols = lax.broadcasted_iota(jnp.int32, (size, size), 1)
    angle = (rows * cols % size).astype(jnp.float32) * (2.0 * math.pi / size)
    return (jnp.cos(angle), jnp.sin(angle))


def toeplitz(kernels):
    width = kernels.shape[-1]
    tail = jnp.zeros(kernels.shape[:-1] + (width + 1,), kernels.dtype)
    padded = jnp.concatenate([kernels, tail], -1)
    tiled = jnp.tile(padded, (1, 1, width))[..., : 2 * width * width]
    return tiled.reshape(kernels.shape[:-1] + (width, 2 * width))


def take_blocks(joined, start):
    return lax.dynamic_slice_in_dim(joined, start, joined.shape[0] // 2, 0)


def slide(joined, starts):
    return jax.vmap(jax.vmap(take_blocks))(joined, starts)


def spread_body(samples, kernels, offsets, weight_index, level_weights):
    segs, comps, rows_one, cols_two = samples.shape
    ranks = lax.axis_size("freq")
    here = lax.axis_index("freq")
    size_one = rows_one * ranks
    length = size_one * cols_two
    highest = lax.Precision.HIGHEST
    cos_two, sin_two = dft_table(cols_two)
    stacked = samples.reshape(segs * comps * rows_one, cols_two)
    with_cos = jnp.dot(stacked, cos_two, precision=highest).reshape(samples.shape)
    with_sin = jnp.dot(stacked, sin_two, precision=highest).reshape(samples.shape)
    first_real = with_cos[:, 0] + with_sin[:, 1]
    first_imag = with_cos[:, 1] - with_sin[:, 0]
    row_global = here * rows_one + lax.broadcasted_iota(jnp.int32, (rows_one, cols_two), 0)
    col_global = lax.broadcasted_iota(jnp.int32, (rows_one, cols_two), 1)
    twist = (row_global * col_global % length).astype(jnp.float32) * (2.0 * math.pi / length)
    twist_cos = jnp.cos(twist)
    twist_sin = jnp.sin(twist)
    turned = jnp.stack(
        [
            first_real * twist_cos + first_imag * twist_sin,
            first_imag * twist_cos - first_real * twist_sin,
        ],
        1,
    )
    columns = lax.all_to_all(
        turned.astype(jnp.bfloat16), "freq", split_axis=3, concat_axis=3, tiled=True
    ).astype(turned.dtype)
    width_two = cols_two // ranks
    ordered = columns.reshape(segs, comps, rows_one, ranks, width_two)
    cos_one, sin_one = dft_table(size_one)
    cos_one = cos_one.reshape(ranks, rows_one, size_one)
    sin_one = sin_one.reshape(ranks, rows_one, size_one)
    second_cos = jnp.einsum("scirl,rik->sclk", ordered, cos_one, precision=highest)
    second_sin = jnp.einsum("scirl,rik->sclk", ordered, sin_one, precision=highest)
    second = jnp.stack(
        [second_cos[:, 0] + second_sin[:, 1], second_cos[:, 1] - second_sin[:, 0]], 1
    )
    arrived = lax.all_to_all(
        second.astype(jnp.bfloat16), "freq", split_axis=3, concat_axis=3, tiled=True
    ).astype(second.dtype)
    width_one = size_one // ranks
    spectrum = arrived.reshape(segs, comps, width_two, ranks, width_one)
    spectrum = jnp.transpose(spectrum, (0, 1, 4, 3, 2)).reshape(segs, comps, width_one * cols_two)
    spectrum = (spectrum * (1.0 / math.sqrt(length))).astype(jnp.bfloat16)
    half = BLOCK // 2
    edged = extended(spectrum, (("freq", 2),), half)
    bins_here = spectrum.shape[2]
    count = bins_here // BLOCK
    lower = edged[..., :bins_here].reshape(segs, comps, count, BLOCK)
    upper = edged[..., BLOCK:].reshape(segs, comps, count, BLOCK)
    window = jnp.concatenate([lower, upper], -1)
    bands = toeplitz(kernels)
    real_band = bands[0]
    imag_band = bands[1]
    table = jnp.stack(
        [jnp.stack([real_band, imag_band], 0), jnp.stack([-imag_band, real_band], 0)], 0
    )
    filtered = jnp.einsum("scbm,cokim->skboi", window, table, preferred_element_type=jnp.float32)
    power = (filtered[:, :, :, 0] ** 2 + filtered[:, :, :, 1] ** 2).astype(jnp.bfloat16)
    quotient = jnp.floor_divide(offsets, count)
    remainder = offsets - quotient * count
    following = passed_along(power, "freq", -1)
    inner = slide(jnp.concatenate([power, following], 2), remainder)
    plane_count = segs * KERNELS
    flat = inner.reshape(plane_count, count * BLOCK)
    plane_quot = quotient.reshape(plane_count)
    distances = lax.broadcasted_iota(jnp.int32, (2 * REACH + 1, plane_count), 0) - REACH
    member = (plane_quot[None, :] == distances).astype(jnp.int32)
    place = jnp.cumsum(member, 1) - 1
    slot_ids = lax.broadcasted_iota(jnp.int32, (2 * REACH + 1, ROUTE_CAP, plane_count), 1)
    select = ((member[:, None, :] == 1) & (place[:, None, :] == slot_ids)).astype(jnp.bfloat16)
    packed = jnp.einsum("dcp,pl->dcl", select, flat, preferred_element_type=jnp.float32).astype(
        jnp.bfloat16
    )
    received = []
    for step_index in range(2 * REACH + 1):
        received.append(passed_along(packed[step_index], "freq", -(step_index - REACH)))
    gathered = jnp.stack(received, 0)
    placed = jnp.einsum("dcp,dcl->pl", select, gathered, preferred_element_type=jnp.float32)
    shifted = placed.astype(jnp.bfloat16).reshape(segs, KERNELS, count, BLOCK)
    levels = lax.broadcasted_iota(jnp.int32, (segs, level_weights.shape[0]), 1)
    weights = jnp.sum(jnp.where(weight_index[:, None] == levels, level_weights[None, :], 0.0), 1)
    scale = 1.0 / (segs * lax.axis_size("seg"))
    partial_sum = jnp.sum((weights * scale)[:, None, None, None] * shifted.astype(jnp.float32), 0)
    owned = lax.psum_scatter(
        partial_sum.astype(jnp.bfloat16), "seg", scatter_dimension=0, tiled=True
    ).astype(jnp.float32)
    return owned.reshape(owned.shape[0], count * BLOCK)


LINE = 4
PAIR = 2
SUB = 16
GROUP = 32


def phases(products, size):
    angle = (np.asarray(products, np.int64) % size) * (2.0 * math.pi / size)
    return np.cos(angle).astype(np.float32), (-np.sin(angle)).astype(np.float32)


def times(a, b):
    return a[0] * b[0] - a[1] * b[1], a[0] * b[1] + a[1] * b[0]


def vmem():
    return pl.BlockSpec(memory_space=pltpu.VMEM)


def smem():
    return pl.BlockSpec(memory_space=pltpu.SMEM)


def anywhere():
    return pl.BlockSpec(memory_space=pl.ANY)


def first_kernel(here, x, ar, ai, br, bi, tr, ti, ur, ui, out, er, ei):
    segs, comps, rows, cols = x.shape
    fine = br.shape[0]
    for coarse in range(ar.shape[0]):
        one = (ar[coarse : coarse + 1, :], ai[coarse : coarse + 1, :])
        real, imag = times(one, (br[...], bi[...]))
        er[pl.ds(coarse * fine, fine), :] = real.astype(jnp.bfloat16)
        ei[pl.ds(coarse * fine, fine), :] = imag.astype(jnp.bfloat16)
    series = x[...].astype(jnp.bfloat16).reshape(segs * comps * rows, cols)
    with_real = jnp.dot(series, er[...], preferred_element_type=jnp.float32)
    with_imag = jnp.dot(series, ei[...], preferred_element_type=jnp.float32)
    sub = ur.shape[0]
    for coarse in range(rows // sub):
        turn = times(
            (tr[here[0], coarse : coarse + 1, :], ti[here[0], coarse : coarse + 1, :]),
            (ur[...], ui[...]),
        )
        for seg in range(segs):
            low = 2 * seg * rows + coarse * sub
            high = low + rows
            value = (
                with_real[low : low + sub] - with_imag[high : high + sub],
                with_imag[low : low + sub] + with_real[high : high + sub],
            )
            real, imag = times(value, turn)
            out[seg, 0, pl.ds(coarse * sub, sub), :] = real.astype(jnp.bfloat16)
            out[seg, 1, pl.ds(coarse * sub, sub), :] = imag.astype(jnp.bfloat16)


def first_stage(samples, here, columns, size_one, scale):
    segs, comps, rows, length = samples.shape
    ranks = size_one // rows
    cols = columns.size
    coarse_table = phases(np.arange(length // GROUP)[:, None] * GROUP * columns[None], length)
    fine_table = phases(np.arange(GROUP)[:, None] * columns[None], length)
    outer = np.arange(size_one // SUB)[:, None] * SUB * columns[None]
    outer = [
        (table * np.float32(scale)).reshape(ranks, rows // SUB, cols)
        for table in phases(outer, size_one * length)
    ]
    inner = phases(np.arange(SUB)[:, None] * columns[None], size_one * length)
    return pl.pallas_call(
        first_kernel,
        out_shape=jax.ShapeDtypeStruct((segs, comps, rows, cols), jnp.bfloat16),
        in_specs=[smem()] + [vmem()] * 9,
        out_specs=vmem(),
        scratch_shapes=[pltpu.VMEM((length, cols), jnp.bfloat16)] * 2,
        name="first_stage",
    )(here, samples, *coarse_table, *fine_table, *outer, *inner)


def gathered(own):
    near = [(i, i ^ PAIR) for i in range(PAIR * LINE)]
    far = [(i, i ^ (2 * PAIR)) for i in range(PAIR * LINE)]
    flip = [(i, i ^ 1) for i in range(PAIR * LINE)]
    middle = [(i, i ^ (3 * PAIR)) for i in range(PAIR, 3 * PAIR)]
    ends = [(i, i ^ PAIR) for i in range(PAIR, 3 * PAIR)]
    half = own.shape[0] // 2
    by_far = lax.ppermute(own, "freq", far)
    by_near = lax.ppermute(own, "freq", near)
    by_flip = lax.ppermute(own, "freq", flip)
    crossed = lax.ppermute(own, "freq", middle)
    near_low = lax.ppermute(by_near[:half], "freq", flip)
    near_high = lax.ppermute(by_flip[half:], "freq", near)
    far_flip = lax.ppermute(by_far, "freq", flip)
    relayed = lax.ppermute(by_far, "freq", ends)
    by_cross = crossed + relayed
    cross_flip = lax.ppermute(by_cross, "freq", flip)
    return [
        (0, own, 0),
        (1, by_flip, 0),
        (PAIR, by_near, 0),
        (PAIR + 1, near_low, 0),
        (PAIR + 1, near_high, half),
        (2 * PAIR, by_far, 0),
        (2 * PAIR + 1, far_flip, 0),
        (3 * PAIR, by_cross, 0),
        (3 * PAIR + 1, cross_flip, 0),
    ]


def chunk_kernel(plan, *refs):
    pieces, first, last, outs, segs, kinds = plan
    refs = list(refs)
    here, row_start, row_shift, lane_start, weight = (refs.pop(0) for _ in range(5))
    slots = [refs.pop(0) for _ in pieces]
    cos, sin, table = (refs.pop(0) for _ in range(3))
    before = None if first else refs.pop(0)
    total_in = None if first else refs.pop(0)
    after = refs.pop(0) if last else None
    total = refs.pop(0)
    extra = refs.pop(0)
    lead = refs.pop(0) if first else None
    parts, held, power, sems = refs
    copies = []
    for number, (distance, start, length) in enumerate(pieces):
        place = lax.bitwise_xor(here[0], distance)
        copies.append(
            pltpu.make_async_copy(
                slots[number],
                parts.at[pl.ds(start, length), :, place],
                sems.at[number],
            )
        )
    for copy in copies:
        copy.start()
    if first:
        total[...] = jnp.zeros_like(total)
    else:
        total[...] = total_in[...]
    for copy in copies:
        copy.wait()
    _, comps, ranks, rows, cols = parts.shape
    count = cols // BLOCK
    size = ranks * rows
    wrap = held.shape[3] - size
    for seg in range(segs):
        real = parts[seg, 0].reshape(size, cols)
        imag = parts[seg, 1].reshape(size, cols)

        def product(table_ref, value):
            return jnp.dot(table_ref[...], value, preferred_element_type=jnp.float32)

        pair = (
            product(cos, real) - product(sin, imag),
            product(cos, imag) + product(sin, real),
        )
        for comp in range(2):
            value = pair[comp].astype(jnp.bfloat16)
            for block in range(count):
                one = value[:, block * BLOCK : (block + 1) * BLOCK]
                held[block, seg, comp, :size, :] = one
                held[block, seg, comp, size:, :] = one[:wrap]
    if first:
        lead[...] = held[0]
    if not last:
        extra[...] = held[count - 1]

    def row_block(block, seg, comp, at):
        if block < 0:
            return before[seg, comp, at, :]
        if block == count:
            return after[seg, comp, at, :]
        return held[block, seg, comp, at, :]

    window = power.shape[2]
    for kind in range(kinds):
        lines = []
        for seg in range(segs):
            at = pl.ds(pl.multiple_of(row_start[seg * kinds + kind], SUB), window)
            for block, _ in outs:
                lines.append(
                    jnp.concatenate(
                        [
                            row_block(block, seg, 0, at),
                            row_block(block + 1, seg, 0, at),
                            row_block(block, seg, 1, at),
                            row_block(block + 1, seg, 1, at),
                        ],
                        1,
                    )
                )
        value = jnp.dot(
            jnp.concatenate(lines, 0), table[kind], preferred_element_type=jnp.float32
        )
        value = value[:, :BLOCK] ** 2 + value[:, BLOCK:] ** 2
        number = 0
        for seg in range(segs):
            plane = seg * kinds + kind
            for _, residue in outs:
                power[kind % 2, number] = value[number * window : (number + 1) * window]
                lane = lane_start[plane]
                carry = jnp.where(residue < lane, 1, 0)
                place = jnp.where(residue < lane, residue - lane + ranks, residue - lane)
                moved = power[kind % 2, number, pl.ds(row_shift[plane] + carry, rows), :]
                total[kind, place] = total[kind, place] + weight[seg] * moved
                number += 1
    if last:
        owned = kinds // 2
        at = owned * (1 - here[1])
        for kind in range(owned):
            extra[kind] = total[at + kind].astype(jnp.bfloat16)


def chunk(scalars, slots, tables, carried, residues, first, last):
    own = slots[0][1]
    segs, comps, rows, cols = own.shape
    cos, sin, table = tables
    size = cos.shape[0]
    ranks = size // rows
    kinds = table.shape[0]
    count = cols // BLOCK
    outs = [] if first else [(-1, residues[0] - 1)]
    outs += [(block, residues[0] + block) for block in range(count - 1)]
    if last:
        outs.append((count - 1, residues[-1]))
    window = rows + SUB
    tall = size + rows
    total_shape = jax.ShapeDtypeStruct((kinds, ranks, rows, BLOCK), jnp.float32)
    edge = jax.ShapeDtypeStruct((segs, comps, tall, BLOCK), jnp.bfloat16)
    out_shape = [total_shape]
    if last:
        out_shape.append(
            jax.ShapeDtypeStruct((kinds // 2, ranks, rows, BLOCK), jnp.bfloat16)
        )
    else:
        out_shape.append(edge)
    if first:
        out_shape.append(edge)
    pieces = tuple((distance, start, piece.shape[0]) for distance, piece, start in slots)
    plan = (pieces, first, last, tuple(outs), segs, kinds)
    arrays = [piece for _, piece, _ in slots]
    inputs = [*scalars, *arrays, cos, sin, table, *carried]
    specs = [smem()] * 5 + [anywhere()] * len(slots) + [vmem()] * (3 + len(carried))
    aliases = {} if first else {5 + len(slots) + 3 + 1: 0}
    return pl.pallas_call(
        functools.partial(chunk_kernel, plan),
        out_shape=out_shape,
        in_specs=specs,
        out_specs=[vmem()] * len(out_shape),
        scratch_shapes=[
            pltpu.VMEM((segs, comps, ranks, rows, cols), jnp.bfloat16),
            pltpu.VMEM((count, segs, comps, tall, BLOCK), jnp.bfloat16),
            pltpu.VMEM((2, segs * len(outs), window, BLOCK), jnp.float32),
            pltpu.SemaphoreType.DMA((len(slots),)),
        ],
        input_output_aliases=aliases,
        name="chunk",
    )(*inputs)


def finish_kernel(here, total, other, out):
    owned, ranks, rows, _ = other.shape
    at = owned * here[1]
    for kind in range(owned):
        for place in range(ranks):
            value = total[at + kind, place] + other[kind, place].astype(jnp.float32)
            out[pl.ds(place * owned + kind, rows, stride=ranks * owned), :] = value


def line_body(samples, kernels, offsets, weight_index, level_weights):
    segs, comps, rows, cols_two = samples.shape
    ranks = lax.axis_size("freq")
    size_one = rows * ranks
    length = size_one * cols_two
    kinds = kernels.shape[1]
    blocks_here = length // ranks // BLOCK
    places = jnp.stack([lax.axis_index("freq"), lax.axis_index("seg")]).astype(jnp.int32)
    columns = np.arange(cols_two) - BLOCK // 2
    residues = np.arange(ranks)
    groups = np.array_split(residues, CHUNKS)
    turned = [
        first_stage(
            samples,
            places,
            columns[group[0] * BLOCK : (group[-1] + 1) * BLOCK],
            size_one,
            1.0 / math.sqrt(length),
        )
        for group in groups
    ]
    slots = [gathered(own) for own in turned]

    grid = np.arange(size_one)
    coarse = phases(np.arange(size_one // GROUP)[:, None] * GROUP * grid[None], size_one)
    fine = phases(np.arange(GROUP)[:, None] * grid[None], size_one)
    real, imag = times(
        [jnp.asarray(part)[:, None] for part in coarse],
        [jnp.asarray(part)[None] for part in fine],
    )
    cos = real.reshape(size_one, size_one).astype(jnp.bfloat16)
    sin = imag.reshape(size_one, size_one).astype(jnp.bfloat16)

    bands = toeplitz(kernels)
    real_band = jnp.swapaxes(bands[0], -1, -2)
    imag_band = jnp.swapaxes(bands[1], -1, -2)
    table = jnp.concatenate(
        [
            jnp.concatenate([real_band, imag_band], -1),
            jnp.concatenate([-imag_band, real_band], -1),
        ],
        -2,
    )

    bins = jnp.remainder(
        lax.axis_index("freq") * blocks_here + offsets.reshape(segs * kinds), ranks * blocks_here
    )
    row = bins // ranks
    lane = bins - row * ranks
    row_start = row // SUB * SUB
    levels = lax.broadcasted_iota(jnp.int32, (segs, level_weights.shape[0]), 1)
    weights = jnp.sum(jnp.where(weight_index[:, None] == levels, level_weights[None, :], 0.0), 1)
    weights = weights * (1.0 / (segs * lax.axis_size("seg")))
    scalars = (places, row_start, row - row_start, lane, weights)

    carried = []
    lead = None
    for number, group in enumerate(groups):
        first = number == 0
        last = number == len(groups) - 1
        if last:
            body_rows = lead[:, :, :size_one]
            carried = carried + [
                jnp.concatenate([body_rows[:, :, 1:], lead[:, :, : rows + 1]], 2)
            ]
        result = chunk(
            scalars, slots[number], (cos, sin, table), carried, list(group), first, last
        )
        if first:
            lead = result[2]
        carried = [result[1], result[0]]
    send, total = carried
    swap = [(i, 1 - i) for i in range(2)]
    other = lax.ppermute(send, "seg", swap)
    owned = kinds // 2
    out = pl.pallas_call(
        finish_kernel,
        out_shape=jax.ShapeDtypeStruct((owned * blocks_here, BLOCK), jnp.float32),
        in_specs=[smem(), vmem(), vmem()],
        out_specs=vmem(),
        name="finish",
    )(places, total, other)
    out = jnp.swapaxes(out.reshape(blocks_here, owned, BLOCK), 0, 1)
    return out.reshape(owned, blocks_here * BLOCK)


def solution(mesh):
    in_specs = (
        P(("parts", "seg"), None, "freq", None),
        P(),
        P(("parts", "seg"), None),
        P(("parts", "seg")),
        P(),
    )
    out_specs = P(("parts", "seg"), "freq")
    line = mesh.shape["freq"] == LINE * PAIR and mesh.shape["seg"] == 2

    def body(samples, *others):
        if line and samples.shape[3] == mesh.shape["freq"] * BLOCK:
            return line_body(samples, *others)
        return spread_body(samples, *others)

    return jax.shard_map(body, mesh=mesh, in_specs=in_specs, out_specs=out_specs, check_vma=False)
```

```python
import functools
import math

import jax
import jax.numpy as jnp
import numpy as np
from jax import lax
from jax.experimental import pallas as pl
from jax.experimental.pallas import tpu as pltpu
from jax.sharding import PartitionSpec as P


BLOCK = 128
KERNELS = 8
REACH = 4
ROUTE_CAP = 4
SPLITS = (5,)
FIRST_LIMIT = 60 * 2**20
CHUNK_LIMIT = 34 * 2**20


def extended(cells, sides, width):
    for axis, dim in sides:
        count = lax.axis_size(axis)
        head = lax.slice_in_dim(cells, 0, width, axis=dim)
        tail = lax.slice_in_dim(cells, cells.shape[dim] - width, cells.shape[dim], axis=dim)
        cells = jnp.concatenate(
            [
                lax.ppermute(tail, axis, [(i, (i + 1) % count) for i in range(count)]),
                cells,
                lax.ppermute(head, axis, [((i + 1) % count, i) for i in range(count)]),
            ],
            axis=dim,
        )
    return cells


def passed_along(block, axis, distance):
    devices = range(lax.axis_size(axis))
    route = [((i - distance) % len(devices), i) for i in devices]
    return lax.ppermute(block, axis, route)


def dft_table(size):
    rows = lax.broadcasted_iota(jnp.int32, (size, size), 0)
    cols = lax.broadcasted_iota(jnp.int32, (size, size), 1)
    angle = (rows * cols % size).astype(jnp.float32) * (2.0 * math.pi / size)
    return (jnp.cos(angle), jnp.sin(angle))


def toeplitz(kernels):
    width = kernels.shape[-1]
    tail = jnp.zeros(kernels.shape[:-1] + (width + 1,), kernels.dtype)
    padded = jnp.concatenate([kernels, tail], -1)
    tiled = jnp.tile(padded, (1, 1, width))[..., : 2 * width * width]
    return tiled.reshape(kernels.shape[:-1] + (width, 2 * width))


def take_blocks(joined, start):
    return lax.dynamic_slice_in_dim(joined, start, joined.shape[0] // 2, 0)


def slide(joined, starts):
    return jax.vmap(jax.vmap(take_blocks))(joined, starts)


def spread_body(samples, kernels, offsets, weight_index, level_weights):
    segs, comps, rows_one, cols_two = samples.shape
    ranks = lax.axis_size("freq")
    here = lax.axis_index("freq")
    size_one = rows_one * ranks
    length = size_one * cols_two
    highest = lax.Precision.HIGHEST
    cos_two, sin_two = dft_table(cols_two)
    stacked = samples.reshape(segs * comps * rows_one, cols_two)
    with_cos = jnp.dot(stacked, cos_two, precision=highest).reshape(samples.shape)
    with_sin = jnp.dot(stacked, sin_two, precision=highest).reshape(samples.shape)
    first_real = with_cos[:, 0] + with_sin[:, 1]
    first_imag = with_cos[:, 1] - with_sin[:, 0]
    row_global = here * rows_one + lax.broadcasted_iota(jnp.int32, (rows_one, cols_two), 0)
    col_global = lax.broadcasted_iota(jnp.int32, (rows_one, cols_two), 1)
    twist = (row_global * col_global % length).astype(jnp.float32) * (2.0 * math.pi / length)
    twist_cos = jnp.cos(twist)
    twist_sin = jnp.sin(twist)
    turned = jnp.stack(
        [
            first_real * twist_cos + first_imag * twist_sin,
            first_imag * twist_cos - first_real * twist_sin,
        ],
        1,
    )
    columns = lax.all_to_all(
        turned.astype(jnp.bfloat16), "freq", split_axis=3, concat_axis=3, tiled=True
    ).astype(turned.dtype)
    width_two = cols_two // ranks
    ordered = columns.reshape(segs, comps, rows_one, ranks, width_two)
    cos_one, sin_one = dft_table(size_one)
    cos_one = cos_one.reshape(ranks, rows_one, size_one)
    sin_one = sin_one.reshape(ranks, rows_one, size_one)
    second_cos = jnp.einsum("scirl,rik->sclk", ordered, cos_one, precision=highest)
    second_sin = jnp.einsum("scirl,rik->sclk", ordered, sin_one, precision=highest)
    second = jnp.stack(
        [second_cos[:, 0] + second_sin[:, 1], second_cos[:, 1] - second_sin[:, 0]], 1
    )
    arrived = lax.all_to_all(
        second.astype(jnp.bfloat16), "freq", split_axis=3, concat_axis=3, tiled=True
    ).astype(second.dtype)
    width_one = size_one // ranks
    spectrum = arrived.reshape(segs, comps, width_two, ranks, width_one)
    spectrum = jnp.transpose(spectrum, (0, 1, 4, 3, 2)).reshape(segs, comps, width_one * cols_two)
    spectrum = (spectrum * (1.0 / math.sqrt(length))).astype(jnp.bfloat16)
    half = BLOCK // 2
    edged = extended(spectrum, (("freq", 2),), half)
    bins_here = spectrum.shape[2]
    count = bins_here // BLOCK
    lower = edged[..., :bins_here].reshape(segs, comps, count, BLOCK)
    upper = edged[..., BLOCK:].reshape(segs, comps, count, BLOCK)
    window = jnp.concatenate([lower, upper], -1)
    bands = toeplitz(kernels)
    real_band = bands[0]
    imag_band = bands[1]
    table = jnp.stack(
        [jnp.stack([real_band, imag_band], 0), jnp.stack([-imag_band, real_band], 0)], 0
    )
    filtered = jnp.einsum("scbm,cokim->skboi", window, table, preferred_element_type=jnp.float32)
    power = (filtered[:, :, :, 0] ** 2 + filtered[:, :, :, 1] ** 2).astype(jnp.bfloat16)
    quotient = jnp.floor_divide(offsets, count)
    remainder = offsets - quotient * count
    following = passed_along(power, "freq", -1)
    inner = slide(jnp.concatenate([power, following], 2), remainder)
    plane_count = segs * KERNELS
    flat = inner.reshape(plane_count, count * BLOCK)
    plane_quot = quotient.reshape(plane_count)
    distances = lax.broadcasted_iota(jnp.int32, (2 * REACH + 1, plane_count), 0) - REACH
    member = (plane_quot[None, :] == distances).astype(jnp.int32)
    place = jnp.cumsum(member, 1) - 1
    slot_ids = lax.broadcasted_iota(jnp.int32, (2 * REACH + 1, ROUTE_CAP, plane_count), 1)
    select = ((member[:, None, :] == 1) & (place[:, None, :] == slot_ids)).astype(jnp.bfloat16)
    packed = jnp.einsum("dcp,pl->dcl", select, flat, preferred_element_type=jnp.float32).astype(
        jnp.bfloat16
    )
    received = []
    for step_index in range(2 * REACH + 1):
        received.append(passed_along(packed[step_index], "freq", -(step_index - REACH)))
    gathered = jnp.stack(received, 0)
    placed = jnp.einsum("dcp,dcl->pl", select, gathered, preferred_element_type=jnp.float32)
    shifted = placed.astype(jnp.bfloat16).reshape(segs, KERNELS, count, BLOCK)
    levels = lax.broadcasted_iota(jnp.int32, (segs, level_weights.shape[0]), 1)
    weights = jnp.sum(jnp.where(weight_index[:, None] == levels, level_weights[None, :], 0.0), 1)
    scale = 1.0 / (segs * lax.axis_size("seg"))
    partial_sum = jnp.sum((weights * scale)[:, None, None, None] * shifted.astype(jnp.float32), 0)
    owned = lax.psum_scatter(
        partial_sum.astype(jnp.bfloat16), "seg", scatter_dimension=0, tiled=True
    ).astype(jnp.float32)
    return owned.reshape(owned.shape[0], count * BLOCK)


LINE = 4
PAIR = 2
SUB = 16
GROUP = 32


def phases(products, size):
    angle = (np.asarray(products, np.int64) % size) * (2.0 * math.pi / size)
    return np.cos(angle).astype(np.float32), (-np.sin(angle)).astype(np.float32)


def times(a, b):
    return a[0] * b[0] - a[1] * b[1], a[0] * b[1] + a[1] * b[0]


def vmem():
    return pl.BlockSpec(memory_space=pltpu.VMEM)


def smem():
    return pl.BlockSpec(memory_space=pltpu.SMEM)


def first_kernel(here, x, ar, ai, br, bi, tr, ti, ur, ui, out, er, ei, wr, wi):
    segs, comps, rows, _ = x.shape
    fine = br.shape[0]
    for coarse in range(ar.shape[0]):
        one = (ar[coarse : coarse + 1, :], ai[coarse : coarse + 1, :])
        real, imag = times(one, (br[...], bi[...]))
        er[pl.ds(coarse * fine, fine), :] = real.astype(jnp.bfloat16)
        ei[pl.ds(coarse * fine, fine), :] = imag.astype(jnp.bfloat16)
    step, sub = out.shape[1], out.shape[3]
    series = x[...].astype(jnp.bfloat16).reshape(segs * comps * rows, x.shape[3])
    for table, kept in ((er, wr), (ei, wi)):
        value = jnp.dot(series, table[...], preferred_element_type=jnp.float32)
        for block in range(kept.shape[0]):
            kept[block] = value[:, block * BLOCK : (block + 1) * BLOCK]
    for block in range(wr.shape[0]):
        lanes = slice(block * BLOCK, (block + 1) * BLOCK)
        for turn in range(step):
            twist = times(
                (tr[here[0], turn : turn + 1, lanes], ti[here[0], turn : turn + 1, lanes]),
                (ur[:, lanes], ui[:, lanes]),
            )
            for seg in range(segs):
                low = pl.ds(2 * seg * rows + turn, sub, stride=step)
                high = pl.ds((2 * seg + 1) * rows + turn, sub, stride=step)
                value = (
                    wr[block, low, :] - wi[block, high, :],
                    wi[block, low, :] + wr[block, high, :],
                )
                real, imag = times(value, twist)
                out[seg, turn, 0, :, lanes] = real.astype(jnp.bfloat16)
                out[seg, turn, 1, :, lanes] = imag.astype(jnp.bfloat16)


def first_stage(samples, here, columns, size_one, scale):
    segs, comps, rows, length = samples.shape
    ranks = size_one // rows
    cols = columns.size
    coarse_table = phases(np.arange(length // GROUP)[:, None] * GROUP * columns[None], length)
    fine_table = phases(np.arange(GROUP)[:, None] * columns[None], length)
    outer = np.arange(ranks)[:, None, None] * rows + np.arange(ranks)[None, :, None]
    outer = [
        table * np.float32(scale)
        for table in phases(outer * columns[None, None], size_one * length)
    ]
    sub = rows // ranks
    inner = phases(np.arange(sub)[:, None] * ranks * columns[None], size_one * length)
    return pl.pallas_call(
        first_kernel,
        out_shape=jax.ShapeDtypeStruct((segs, ranks, comps, sub, cols), jnp.bfloat16),
        in_specs=[smem()] + [vmem()] * 9,
        out_specs=vmem(),
        scratch_shapes=[pltpu.VMEM((length, cols), jnp.bfloat16)] * 2
        + [pltpu.VMEM((cols // BLOCK, segs * comps * rows, BLOCK), jnp.float32)] * 2,
        compiler_params=pltpu.CompilerParams(vmem_limit_bytes=FIRST_LIMIT),
        cost_estimate=pl.CostEstimate(
            flops=2 * segs * comps * rows * length * 2 * cols,
            bytes_accessed=4 * samples.size,
            transcendentals=0,
        ),
        name="first_stage",
    )(here, samples, *coarse_table, *fine_table, *outer, *inner)


def gathered(own, tied):
    near = [(i, i ^ PAIR) for i in range(PAIR * LINE)]
    far = [(i, i ^ (2 * PAIR)) for i in range(PAIR * LINE)]
    flip = [(i, i ^ 1) for i in range(PAIR * LINE)]
    middle = [(i, i ^ (3 * PAIR)) for i in range(PAIR, 3 * PAIR)]
    ends = [(i, i ^ PAIR) for i in range(PAIR, 3 * PAIR)]
    half = own.shape[0] // 2

    def send(array, route):
        return lax.ppermute(array, "freq", route)

    by_near = send(own, near)
    crossed = send(own, middle)
    by_flip = send(own, flip)
    by_far = send(own, far)
    low = by_near[:half]
    high = by_flip[half:]
    low, tied = lax.optimization_barrier((low, tied))
    near_low = send(low, flip)
    near_high = send(high, near)
    far_flip = send(by_far, flip)
    relayed = send(by_far, ends)
    by_cross = crossed + relayed
    cross_flip = send(by_cross, flip)
    return [
        (0, own, 0),
        (1, by_flip, 0),
        (PAIR, by_near, 0),
        (PAIR + 1, near_low, 0),
        (PAIR + 1, near_high, half),
        (2 * PAIR, by_far, 0),
        (2 * PAIR + 1, far_flip, 0),
        (3 * PAIR, by_cross, 0),
        (3 * PAIR + 1, cross_flip, 0),
    ], tied


def eight(z):
    root = np.float32(math.sqrt(0.5))

    def add(a, b):
        return a[0] + b[0], a[1] + b[1]

    def sub(a, b):
        return a[0] - b[0], a[1] - b[1]

    def four(a, b, c, d):
        p, q, r, s = add(a, c), sub(a, c), add(b, d), sub(b, d)
        return (
            add(p, r),
            (q[0] + s[1], q[1] - s[0]),
            sub(p, r),
            (q[0] - s[1], q[1] + s[0]),
        )

    even = four(z[0], z[2], z[4], z[6])
    odd = list(four(z[1], z[3], z[5], z[7]))
    x, y = odd[1]
    odd[1] = ((x + y) * root, (y - x) * root)
    x, y = odd[2]
    odd[2] = (y, -x)
    x, y = odd[3]
    odd[3] = ((y - x) * root, -(x + y) * root)
    return [add(even[m], odd[m]) for m in range(4)] + [sub(even[m], odd[m]) for m in range(4)]


def chunk_kernel(plan, *refs):
    pieces, first, last, outs, segs, kinds = plan
    planes = segs * kinds
    refs = list(refs)
    ints, weight = refs.pop(0), refs.pop(0)
    slots = [refs.pop(0) for _ in pieces]
    mats, bands = refs.pop(0), refs.pop(0)
    before = None if first else refs.pop(0)
    total_in = None if first else refs.pop(0)
    after = refs.pop(0) if last else None
    if last:
        mine_out, send_out = refs.pop(0), refs.pop(0)
    else:
        total, edge_out = refs.pop(0), refs.pop(0)
    if first:
        after = refs.pop(0)
    parts, mixed, held, power = (refs.pop(0) for _ in range(4))
    if last:
        total, theirs = refs.pop(0), refs.pop(0)

    def row_start(plane):
        return ints[2 + plane]

    def row_shift(plane):
        return ints[2 + planes + plane]

    def lane_start(plane):
        return ints[2 + 2 * planes + plane]

    for number, (distance, start, length) in enumerate(pieces):
        place = lax.bitwise_xor(ints[0], distance)
        for seg in range(length):
            for turn in range(parts.shape[1]):
                for comp in range(parts.shape[2]):
                    parts[start + seg, turn, comp, place] = slots[number][seg, turn, comp]
    _, step, comps, ranks, sub, cols = parts.shape
    rows = ranks * sub
    count = cols // BLOCK
    size = step * rows
    wrap = held.shape[3] - size
    for seg in range(segs):
        for low in range(0, cols, 2 * BLOCK):
            width = min(2 * BLOCK, cols - low)
            for turn in range(step):
                value = parts[seg, turn, :, :, :, low : low + width]
                mixed[turn, :, :width] = jnp.dot(
                    mats[turn],
                    value.reshape(comps * rows, width),
                    preferred_element_type=jnp.float32,
                )
            for lane in range(0, width, BLOCK):
                block = (low + lane) // BLOCK
                lanes = slice(lane, lane + BLOCK)
                for row in range(0, rows, SUB):
                    z = [
                        (
                            mixed[turn, row : row + SUB, lanes],
                            mixed[turn, rows + row : rows + row + SUB, lanes],
                        )
                        for turn in range(step)
                    ]
                    for turn, value in enumerate(eight(z)):
                        for comp in range(2):
                            one = value[comp].astype(jnp.bfloat16)
                            at = turn * rows + row
                            held[block, seg, comp, at : at + SUB, :] = one
                            if at < wrap:
                                held[block, seg, comp, size + at : size + at + SUB, :] = one
    if not last:
        edge_out[...] = held[count - 1]
    if first:
        for seg in range(segs):
            for comp in range(comps):
                value = held[0, seg, comp, :, :].astype(jnp.float32)
                value = pltpu.roll(value, value.shape[0] - 1, 0).astype(jnp.bfloat16)
                after[seg, comp, :size, :] = value[:size]
                after[seg, comp, size:, :] = value[:wrap]
        total[...] = jnp.zeros_like(total)
    else:
        total[...] = total_in[...]

    def row_block(block, seg, comp, at):
        if block < 0:
            return before[seg, comp, at, :]
        if block == count:
            return after[seg, comp, at, :]
        return held[block, seg, comp, at, :]

    window = power.shape[2]
    for kind in range(kinds):
        real_band, imag_band = bands[0, kind], bands[1, kind]
        table = (
            jnp.concatenate([real_band, imag_band], 1),
            jnp.concatenate([-imag_band, real_band], 1),
        )
        value = None
        for comp in range(2):
            lines = []
            for seg in range(segs):
                at = pl.ds(pl.multiple_of(row_start(seg * kinds + kind), SUB), window)
                for block, _ in outs:
                    lines.append(
                        jnp.concatenate(
                            [row_block(block, seg, comp, at), row_block(block + 1, seg, comp, at)],
                            1,
                        )
                    )
            one = jnp.dot(
                jnp.concatenate(lines, 0), table[comp], preferred_element_type=jnp.float32
            )
            value = one if value is None else value + one
        value = value[:, :BLOCK] ** 2 + value[:, BLOCK:] ** 2
        number = 0
        for seg in range(segs):
            plane = seg * kinds + kind
            lane = lane_start(plane)
            for _, residue in outs:
                power[kind % 2, number] = value[number * window : (number + 1) * window]
                carry = jnp.where(residue < lane, 1, 0)
                place = residue - lane + carry * ranks
                moved = power[kind % 2, number, pl.ds(row_shift(plane) + carry, rows), :]
                total[kind, place] = total[kind, place] + weight[seg] * moved
                number += 1
    if last:
        owned = kinds // 2
        theirs_at = owned * (1 - ints[1])
        mine_at = owned * ints[1]
        for target, base in ((theirs, theirs_at), (mine_out, mine_at)):
            for kind in range(owned):
                for place in range(ranks):
                    at = pl.ds(place * owned + kind, rows, stride=ranks * owned)
                    target[at, :] = total[base + kind, place]
            if target is theirs:
                send_out[...] = theirs[...].astype(jnp.bfloat16)


def chunk(scalars, slots, tables, carried, residues, first, last):
    own = slots[0][1]
    segs, step, comps, sub, cols = own.shape
    ranks = step
    rows = ranks * sub
    size = step * rows
    mats, bands = tables
    kinds = bands.shape[1]
    count = cols // BLOCK
    outs = [] if first else [(-1, residues[0] - 1)]
    outs += [(block, residues[0] + block) for block in range(count - 1)]
    if last:
        outs.append((count - 1, residues[-1]))
    window = rows + SUB
    tall = size + rows
    edge = jax.ShapeDtypeStruct((segs, comps, tall, BLOCK), jnp.bfloat16)
    total = jax.ShapeDtypeStruct((kinds, ranks, rows, BLOCK), jnp.float32)
    flat = (kinds // 2 * ranks * rows, BLOCK)
    if last:
        out_shape = [
            jax.ShapeDtypeStruct(flat, jnp.float32),
            jax.ShapeDtypeStruct(flat, jnp.bfloat16),
        ]
    else:
        out_shape = [total, edge]
    if first:
        out_shape.append(edge)
    pieces = tuple((distance, begin, piece.shape[0]) for distance, piece, begin in slots)
    plan = (pieces, first, last, tuple(outs), segs, kinds)
    arrays = [piece for _, piece, _ in slots]
    inputs = [*scalars, *arrays, mats, bands, *carried]
    specs = [smem()] * 2 + [vmem()] * (len(inputs) - 2)
    scratch = [
        pltpu.VMEM((segs, step, comps, ranks, sub, cols), jnp.bfloat16),
        pltpu.VMEM((step, comps * rows, 2 * BLOCK), jnp.float32),
        pltpu.VMEM((count, segs, comps, tall, BLOCK), jnp.bfloat16),
        pltpu.VMEM((2, segs * len(outs), window, BLOCK), jnp.float32),
    ]
    if last:
        scratch += [pltpu.VMEM(total.shape, total.dtype), pltpu.VMEM(flat, jnp.float32)]
    return pl.pallas_call(
        functools.partial(chunk_kernel, plan),
        out_shape=out_shape,
        in_specs=specs,
        out_specs=[vmem()] * len(out_shape),
        scratch_shapes=scratch,
        compiler_params=pltpu.CompilerParams(vmem_limit_bytes=CHUNK_LIMIT),
        cost_estimate=pl.CostEstimate(
            flops=2 * segs * len(outs) * kinds * window * 4 * BLOCK * 2 * BLOCK
            + 8 * segs * step * rows * rows * cols,
            bytes_accessed=8 * total.size,
            transcendentals=0,
        ),
        name="chunk",
    )(*inputs)


def line_body(samples, kernels, offsets, weight_index, level_weights):
    segs, _, rows, cols_two = samples.shape
    ranks = lax.axis_size("freq")
    size_one = rows * ranks
    length = size_one * cols_two
    kinds = kernels.shape[1]
    blocks_here = length // ranks // BLOCK
    places = jnp.stack([lax.axis_index("freq"), lax.axis_index("seg")]).astype(jnp.int32)
    columns = np.arange(cols_two) - BLOCK // 2
    groups = np.split(np.arange(ranks), SPLITS)
    turned = []
    for group in groups:
        turned.append(
            first_stage(
                samples,
                places,
                columns[group[0] * BLOCK : (group[-1] + 1) * BLOCK],
                size_one,
                1.0 / math.sqrt(length),
            )
        )

    times_of = np.arange(ranks)[:, None, None] + ranks * np.arange(rows)[None, None, :]
    real, imag = phases(times_of * np.arange(rows)[None, :, None], size_one)
    mats = np.concatenate(
        [np.concatenate([real, -imag], 2), np.concatenate([imag, real], 2)], 1
    ).astype(jnp.bfloat16)
    bands = jnp.swapaxes(toeplitz(kernels), -1, -2)

    slots = []
    for own in turned:
        pieces, bands = gathered(own, bands)
        slots.append(pieces)

    bins = jnp.remainder(
        lax.axis_index("freq") * blocks_here + offsets.reshape(segs * kinds), ranks * blocks_here
    )
    row = bins // ranks
    lane = bins - row * ranks
    row_start = row // SUB * SUB
    ints = jnp.concatenate([places, row_start, row - row_start, lane])
    levels = lax.broadcasted_iota(jnp.int32, (segs, level_weights.shape[0]), 1)
    weights = jnp.sum(jnp.where(weight_index[:, None] == levels, level_weights[None, :], 0.0), 1)
    weights = weights * (1.0 / (segs * lax.axis_size("seg")))
    scalars = (ints, weights)

    carried = []
    rolled = None
    for number, group in enumerate(groups):
        first = number == 0
        last = number == len(groups) - 1
        if last:
            carried = carried + [rolled]
        result = chunk(
            scalars, slots[number], (mats, bands), carried, list(group), first, last
        )
        if first:
            rolled = result[2]
        carried = [result[1], result[0]]
    send, own = carried
    other = lax.ppermute(send, "seg", [(i, 1 - i) for i in range(2)])
    out = own + other.astype(jnp.float32)
    owned = kinds // 2
    out = jnp.swapaxes(out.reshape(blocks_here, owned, BLOCK), 0, 1)
    return out.reshape(owned, blocks_here * BLOCK)


def solution(mesh):
    in_specs = (
        P(("parts", "seg"), None, "freq", None),
        P(),
        P(("parts", "seg"), None),
        P(("parts", "seg")),
        P(),
    )
    out_specs = P(("parts", "seg"), "freq")
    line = mesh.shape["freq"] == LINE * PAIR and mesh.shape["seg"] == 2

    def body(samples, *others):
        if not line:
            return spread_body(samples, *others)
        return line_body(samples, *others)

    return jax.shard_map(body, mesh=mesh, in_specs=in_specs, out_specs=out_specs, check_vma=False)
```

```python
import functools
import math

import jax
import jax.numpy as jnp
import numpy as np
from jax import lax
from jax.experimental import pallas as pl
from jax.experimental.pallas import tpu as pltpu
from jax.sharding import PartitionSpec as P


BLOCK = 128
KERNELS = 8
REACH = 4
ROUTE_CAP = 4
SPLITS = (4,)
FIRST_LIMIT = 60 * 2**20
CHUNK_LIMIT = 34 * 2**20


def extended(cells, sides, width):
    for axis, dim in sides:
        count = lax.axis_size(axis)
        head = lax.slice_in_dim(cells, 0, width, axis=dim)
        tail = lax.slice_in_dim(cells, cells.shape[dim] - width, cells.shape[dim], axis=dim)
        cells = jnp.concatenate(
            [
                lax.ppermute(tail, axis, [(i, (i + 1) % count) for i in range(count)]),
                cells,
                lax.ppermute(head, axis, [((i + 1) % count, i) for i in range(count)]),
            ],
            axis=dim,
        )
    return cells


def passed_along(block, axis, distance):
    devices = range(lax.axis_size(axis))
    route = [((i - distance) % len(devices), i) for i in devices]
    return lax.ppermute(block, axis, route)


def dft_table(size):
    rows = lax.broadcasted_iota(jnp.int32, (size, size), 0)
    cols = lax.broadcasted_iota(jnp.int32, (size, size), 1)
    angle = (rows * cols % size).astype(jnp.float32) * (2.0 * math.pi / size)
    return (jnp.cos(angle), jnp.sin(angle))


def toeplitz(kernels):
    width = kernels.shape[-1]
    tail = jnp.zeros(kernels.shape[:-1] + (width + 1,), kernels.dtype)
    padded = jnp.concatenate([kernels, tail], -1)
    tiled = jnp.tile(padded, (1, 1, width))[..., : 2 * width * width]
    return tiled.reshape(kernels.shape[:-1] + (width, 2 * width))


def take_blocks(joined, start):
    return lax.dynamic_slice_in_dim(joined, start, joined.shape[0] // 2, 0)


def slide(joined, starts):
    return jax.vmap(jax.vmap(take_blocks))(joined, starts)


def spread_body(samples, kernels, offsets, weight_index, level_weights):
    segs, comps, rows_one, cols_two = samples.shape
    ranks = lax.axis_size("freq")
    here = lax.axis_index("freq")
    size_one = rows_one * ranks
    length = size_one * cols_two
    highest = lax.Precision.HIGHEST
    cos_two, sin_two = dft_table(cols_two)
    stacked = samples.reshape(segs * comps * rows_one, cols_two)
    with_cos = jnp.dot(stacked, cos_two, precision=highest).reshape(samples.shape)
    with_sin = jnp.dot(stacked, sin_two, precision=highest).reshape(samples.shape)
    first_real = with_cos[:, 0] + with_sin[:, 1]
    first_imag = with_cos[:, 1] - with_sin[:, 0]
    row_global = here * rows_one + lax.broadcasted_iota(jnp.int32, (rows_one, cols_two), 0)
    col_global = lax.broadcasted_iota(jnp.int32, (rows_one, cols_two), 1)
    twist = (row_global * col_global % length).astype(jnp.float32) * (2.0 * math.pi / length)
    twist_cos = jnp.cos(twist)
    twist_sin = jnp.sin(twist)
    turned = jnp.stack(
        [
            first_real * twist_cos + first_imag * twist_sin,
            first_imag * twist_cos - first_real * twist_sin,
        ],
        1,
    )
    columns = lax.all_to_all(
        turned.astype(jnp.bfloat16), "freq", split_axis=3, concat_axis=3, tiled=True
    ).astype(turned.dtype)
    width_two = cols_two // ranks
    ordered = columns.reshape(segs, comps, rows_one, ranks, width_two)
    cos_one, sin_one = dft_table(size_one)
    cos_one = cos_one.reshape(ranks, rows_one, size_one)
    sin_one = sin_one.reshape(ranks, rows_one, size_one)
    second_cos = jnp.einsum("scirl,rik->sclk", ordered, cos_one, precision=highest)
    second_sin = jnp.einsum("scirl,rik->sclk", ordered, sin_one, precision=highest)
    second = jnp.stack(
        [second_cos[:, 0] + second_sin[:, 1], second_cos[:, 1] - second_sin[:, 0]], 1
    )
    arrived = lax.all_to_all(
        second.astype(jnp.bfloat16), "freq", split_axis=3, concat_axis=3, tiled=True
    ).astype(second.dtype)
    width_one = size_one // ranks
    spectrum = arrived.reshape(segs, comps, width_two, ranks, width_one)
    spectrum = jnp.transpose(spectrum, (0, 1, 4, 3, 2)).reshape(segs, comps, width_one * cols_two)
    spectrum = (spectrum * (1.0 / math.sqrt(length))).astype(jnp.bfloat16)
    half = BLOCK // 2
    edged = extended(spectrum, (("freq", 2),), half)
    bins_here = spectrum.shape[2]
    count = bins_here // BLOCK
    lower = edged[..., :bins_here].reshape(segs, comps, count, BLOCK)
    upper = edged[..., BLOCK:].reshape(segs, comps, count, BLOCK)
    window = jnp.concatenate([lower, upper], -1)
    bands = toeplitz(kernels)
    real_band = bands[0]
    imag_band = bands[1]
    table = jnp.stack(
        [jnp.stack([real_band, imag_band], 0), jnp.stack([-imag_band, real_band], 0)], 0
    )
    filtered = jnp.einsum("scbm,cokim->skboi", window, table, preferred_element_type=jnp.float32)
    power = (filtered[:, :, :, 0] ** 2 + filtered[:, :, :, 1] ** 2).astype(jnp.bfloat16)
    quotient = jnp.floor_divide(offsets, count)
    remainder = offsets - quotient * count
    following = passed_along(power, "freq", -1)
    inner = slide(jnp.concatenate([power, following], 2), remainder)
    plane_count = segs * KERNELS
    flat = inner.reshape(plane_count, count * BLOCK)
    plane_quot = quotient.reshape(plane_count)
    distances = lax.broadcasted_iota(jnp.int32, (2 * REACH + 1, plane_count), 0) - REACH
    member = (plane_quot[None, :] == distances).astype(jnp.int32)
    place = jnp.cumsum(member, 1) - 1
    slot_ids = lax.broadcasted_iota(jnp.int32, (2 * REACH + 1, ROUTE_CAP, plane_count), 1)
    select = ((member[:, None, :] == 1) & (place[:, None, :] == slot_ids)).astype(jnp.bfloat16)
    packed = jnp.einsum("dcp,pl->dcl", select, flat, preferred_element_type=jnp.float32).astype(
        jnp.bfloat16
    )
    received = []
    for step_index in range(2 * REACH + 1):
        received.append(passed_along(packed[step_index], "freq", -(step_index - REACH)))
    gathered = jnp.stack(received, 0)
    placed = jnp.einsum("dcp,dcl->pl", select, gathered, preferred_element_type=jnp.float32)
    shifted = placed.astype(jnp.bfloat16).reshape(segs, KERNELS, count, BLOCK)
    levels = lax.broadcasted_iota(jnp.int32, (segs, level_weights.shape[0]), 1)
    weights = jnp.sum(jnp.where(weight_index[:, None] == levels, level_weights[None, :], 0.0), 1)
    scale = 1.0 / (segs * lax.axis_size("seg"))
    partial_sum = jnp.sum((weights * scale)[:, None, None, None] * shifted.astype(jnp.float32), 0)
    owned = lax.psum_scatter(
        partial_sum.astype(jnp.bfloat16), "seg", scatter_dimension=0, tiled=True
    ).astype(jnp.float32)
    return owned.reshape(owned.shape[0], count * BLOCK)


LINE = 4
PAIR = 2
SUB = 16
GROUP = 32


def phases(products, size):
    angle = (np.asarray(products, np.int64) % size) * (2.0 * math.pi / size)
    return np.cos(angle).astype(np.float32), (-np.sin(angle)).astype(np.float32)


def times(a, b):
    return a[0] * b[0] - a[1] * b[1], a[0] * b[1] + a[1] * b[0]


def vmem():
    return pl.BlockSpec(memory_space=pltpu.VMEM)


def smem():
    return pl.BlockSpec(memory_space=pltpu.SMEM)


def first_kernel(begin, heights, x_hbm, tables_hbm, out, x, tables, er, ei, wr, wi, sems):
    segs, comps, rows, length = x.shape
    step, sub, cols = out.shape[1], out.shape[3], out.shape[4]
    copies = [
        pltpu.make_async_copy(tables_hbm.at[:, pl.ds(begin, cols)], tables, sems.at[segs])
    ]
    for seg in range(segs):
        copies.append(pltpu.make_async_copy(x_hbm.at[seg], x.at[seg], sems.at[seg]))
    for copy in copies:
        copy.start()
    here = lax.axis_index("freq")
    at = np.concatenate([[0], np.cumsum(heights)])

    def table(number, row=0, height=None):
        height = heights[number] if height is None else height
        return tables[pl.ds(int(at[number]) + row, height), :]

    fine = heights[2]
    copies[0].wait()
    inner = (table(2), table(3))
    for coarse in range(heights[0]):
        real, imag = times((table(0, coarse, 1), table(1, coarse, 1)), inner)
        er[pl.ds(coarse * fine, fine), :] = real.astype(jnp.bfloat16)
        ei[pl.ds(coarse * fine, fine), :] = imag.astype(jnp.bfloat16)
    for seg in range(segs):
        copies[1 + seg].wait()
        series = x[seg].astype(jnp.bfloat16).reshape(comps * rows, length)
        for phase, kept in ((er, wr), (ei, wi)):
            value = jnp.dot(series, phase[...], preferred_element_type=jnp.float32)
            for block in range(kept.shape[1]):
                kept[seg, block] = value[:, block * BLOCK : (block + 1) * BLOCK]
        for block in range(wr.shape[1]):
            lanes = slice(block * BLOCK, (block + 1) * BLOCK)
            turned = (table(6)[:, lanes], table(7)[:, lanes])
            for turn in range(step):
                row = here * step + turn
                twist = times((table(4, row, 1)[:, lanes], table(5, row, 1)[:, lanes]), turned)
                low = pl.ds(turn, sub, stride=step)
                high = pl.ds(rows + turn, sub, stride=step)
                value = (
                    wr[seg, block, low, :] - wi[seg, block, high, :],
                    wi[seg, block, low, :] + wr[seg, block, high, :],
                )
                real, imag = times(value, twist)
                out[seg, turn, 0, :, lanes] = real.astype(jnp.bfloat16)
                out[seg, turn, 1, :, lanes] = imag.astype(jnp.bfloat16)


def first_tables(samples, ranks):
    _, _, rows, length = samples.shape
    columns = np.arange(length) - BLOCK // 2
    size = rows * ranks * length
    scale = np.float32(1.0 / math.sqrt(size))
    coarse = phases(np.arange(length // GROUP)[:, None] * GROUP * columns[None], length)
    fine = phases(np.arange(GROUP)[:, None] * columns[None], length)
    outer = np.arange(ranks)[:, None] * rows + np.arange(ranks)[None]
    outer = [scale * part for part in phases(outer.reshape(-1, 1) * columns[None], size)]
    inner = phases(np.arange(rows // ranks)[:, None] * ranks * columns[None], size)
    parts = [*coarse, *fine, *outer, *inner]
    return tuple(part.shape[0] for part in parts), np.concatenate(parts, 0)


def first_stage(samples, heights, tables, ranks, begin, cols):
    segs, comps, rows, length = samples.shape
    sub = rows // ranks
    return pl.pallas_call(
        functools.partial(first_kernel, begin, heights),
        out_shape=jax.ShapeDtypeStruct((segs, ranks, comps, sub, cols), jnp.bfloat16),
        in_specs=[pl.BlockSpec(memory_space=pl.ANY)] * 2,
        out_specs=vmem(),
        scratch_shapes=[
            pltpu.VMEM(samples.shape, samples.dtype),
            pltpu.VMEM((tables.shape[0], cols), tables.dtype),
        ]
        + [pltpu.VMEM((length, cols), jnp.bfloat16)] * 2
        + [pltpu.VMEM((segs, cols // BLOCK, comps * rows, BLOCK), jnp.float32)] * 2
        + [pltpu.SemaphoreType.DMA((segs + 1,))],
        compiler_params=pltpu.CompilerParams(vmem_limit_bytes=FIRST_LIMIT),
        cost_estimate=pl.CostEstimate(
            flops=2 * segs * comps * rows * length * 2 * cols,
            bytes_accessed=4 * samples.size,
            transcendentals=0,
        ),
        name="first_stage",
    )(samples, tables)


def gathered(own):
    near = [(i, i ^ PAIR) for i in range(PAIR * LINE)]
    far = [(i, i ^ (2 * PAIR)) for i in range(PAIR * LINE)]
    flip = [(i, i ^ 1) for i in range(PAIR * LINE)]
    middle = [(i, i ^ (3 * PAIR)) for i in range(PAIR, 3 * PAIR)]
    ends = [(i, i ^ PAIR) for i in range(PAIR, 3 * PAIR)]
    half = own.shape[0] // 2

    def send(array, route):
        return lax.ppermute(array, "freq", route)

    by_near = send(own, near)
    crossed = send(own, middle)
    by_flip = send(own, flip)
    by_far = send(own, far)
    low = by_near[:half]
    high = by_flip[half:]
    near_low = send(low, flip)
    near_high = send(high, near)
    far_flip = send(by_far, flip)
    relayed = send(by_far, ends)
    flip_middle = send(crossed, [pair for pair in flip if pair[0] in dict(middle)])
    flip_ends = send(relayed, [pair for pair in flip if pair[0] not in dict(middle)])
    return [
        (0, 0, own),
        (1, 0, by_flip),
        (PAIR, 0, by_near),
        (PAIR + 1, 0, near_low),
        (PAIR + 1, half, near_high),
        (2 * PAIR, 0, by_far),
        (2 * PAIR + 1, 0, far_flip),
        (3 * PAIR, 0, crossed, relayed),
        (3 * PAIR + 1, 0, flip_middle, flip_ends),
    ]


def eight(z):
    root = np.float32(math.sqrt(0.5))

    def add(a, b):
        return a[0] + b[0], a[1] + b[1]

    def sub(a, b):
        return a[0] - b[0], a[1] - b[1]

    def four(a, b, c, d):
        p, q, r, s = add(a, c), sub(a, c), add(b, d), sub(b, d)
        return (
            add(p, r),
            (q[0] + s[1], q[1] - s[0]),
            sub(p, r),
            (q[0] - s[1], q[1] + s[0]),
        )

    even = four(z[0], z[2], z[4], z[6])
    odd = list(four(z[1], z[3], z[5], z[7]))
    x, y = odd[1]
    odd[1] = ((x + y) * root, (y - x) * root)
    x, y = odd[2]
    odd[2] = (y, -x)
    x, y = odd[3]
    odd[3] = ((y - x) * root, -(x + y) * root)
    return [add(even[m], odd[m]) for m in range(4)] + [sub(even[m], odd[m]) for m in range(4)]


def chunk_kernel(plan, *refs):
    pieces, first, last, outs, segs, kinds = plan
    planes = segs * kinds
    refs = list(refs)
    ints, weight = refs.pop(0), refs.pop(0)
    slots = [[refs.pop(0) for _ in range(many)] for _, _, many in pieces]
    mats, bands = refs.pop(0), refs.pop(0)
    before = None if first else refs.pop(0)
    total_in = None if first else refs.pop(0)
    after = refs.pop(0) if last else None
    if last:
        mine_out, send_out = refs.pop(0), refs.pop(0)
    else:
        total, edge_out = refs.pop(0), refs.pop(0)
    if first:
        after = refs.pop(0)
    parts, mixed, held, power = (refs.pop(0) for _ in range(4))
    if last:
        total = refs.pop(0)

    def row_start(plane):
        return ints[2 + plane]

    def row_shift(plane):
        return ints[2 + planes + plane]

    def lane_start(plane):
        return ints[2 + 2 * planes + plane]

    for (distance, start, _), arrays in zip(pieces, slots):
        place = lax.bitwise_xor(ints[0], distance)
        for seg in range(arrays[0].shape[0]):
            for turn in range(parts.shape[1]):
                for comp in range(parts.shape[2]):
                    value = arrays[0][seg, turn, comp]
                    for other in arrays[1:]:
                        value = value + other[seg, turn, comp]
                    parts[start + seg, turn, comp, place] = value
    _, step, comps, ranks, sub, cols = parts.shape
    rows = ranks * sub
    count = cols // BLOCK
    size = step * rows
    wrap = held.shape[3] - size
    for seg in range(segs):
        for low in range(0, cols, 2 * BLOCK):
            width = min(2 * BLOCK, cols - low)
            for turn in range(step):
                value = parts[seg, turn, :, :, :, low : low + width]
                mixed[turn, :, :width] = jnp.dot(
                    mats[turn],
                    value.reshape(comps * rows, width),
                    preferred_element_type=jnp.float32,
                )
            for lane in range(0, width, BLOCK):
                block = (low + lane) // BLOCK
                lanes = slice(lane, lane + BLOCK)
                for row in range(0, rows, SUB):
                    z = [
                        (
                            mixed[turn, row : row + SUB, lanes],
                            mixed[turn, rows + row : rows + row + SUB, lanes],
                        )
                        for turn in range(step)
                    ]
                    for turn, value in enumerate(eight(z)):
                        for comp in range(2):
                            one = value[comp].astype(jnp.bfloat16)
                            at = turn * rows + row
                            held[block, seg, comp, at : at + SUB, :] = one
                            if at < wrap:
                                held[block, seg, comp, size + at : size + at + SUB, :] = one
    if not last:
        edge_out[...] = held[count - 1]
    if first:
        for seg in range(segs):
            for comp in range(comps):
                value = held[0, seg, comp, :, :].astype(jnp.float32)
                value = pltpu.roll(value, value.shape[0] - 1, 0).astype(jnp.bfloat16)
                after[seg, comp, :size, :] = value[:size]
                after[seg, comp, size:, :] = value[:wrap]
        total[...] = jnp.zeros_like(total)
    else:
        total[...] = total_in[...]

    def row_block(block, seg, comp, at):
        if block < 0:
            return before[seg, comp, at, :]
        if block == count:
            return after[seg, comp, at, :]
        return held[block, seg, comp, at, :]

    window = power.shape[2]
    for kind in range(kinds):
        real_band, imag_band = bands[0, kind], bands[1, kind]
        table = (
            jnp.concatenate([real_band, imag_band], 1),
            jnp.concatenate([-imag_band, real_band], 1),
        )
        lines = []
        for seg in range(segs):
            at = pl.ds(pl.multiple_of(row_start(seg * kinds + kind), SUB), window)
            for block, _ in outs:
                lines.append(
                    jnp.concatenate(
                        [
                            row_block(block + side, seg, comp, at)
                            for comp in range(2)
                            for side in range(2)
                        ],
                        1,
                    )
                )
        value = jnp.dot(
            jnp.concatenate(lines, 0),
            jnp.concatenate(table, 0),
            preferred_element_type=jnp.float32,
        )
        value = value[:, :BLOCK] ** 2 + value[:, BLOCK:] ** 2
        number = 0
        for seg in range(segs):
            plane = seg * kinds + kind
            lane = lane_start(plane)
            for _, residue in outs:
                power[kind % 2, number] = value[number * window : (number + 1) * window]
                carry = jnp.where(residue < lane, 1, 0)
                place = residue - lane + carry * ranks
                moved = power[kind % 2, number, pl.ds(row_shift(plane) + carry, rows), :]
                total[kind, place] = total[kind, place] + weight[seg] * moved
                number += 1
    if last:
        owned = kinds // 2
        theirs_at = owned * (1 - ints[1])
        mine_at = owned * ints[1]
        lane_rows = 8
        for target, base in ((send_out, theirs_at), (mine_out, mine_at)):
            for row in range(0, rows, lane_rows):
                tiles = [
                    total[base + kind, place, row : row + lane_rows, :]
                    for place in range(ranks)
                    for kind in range(owned)
                ]
                value = jnp.swapaxes(jnp.stack(tiles, 0), 0, 1).reshape(-1, BLOCK)
                height = value.shape[0]
                at = row // lane_rows * height
                target[at : at + height, :] = value.astype(target.dtype)


def bands_kernel(kernels, out):
    comps, kinds, width = kernels.shape
    for comp in range(comps):
        for kind in range(kinds):
            row = kernels[comp, kind : kind + 1, :].astype(jnp.float32)
            rows = jnp.broadcast_to(jnp.concatenate([row, jnp.zeros_like(row)], 1), (width, 2 * width))
            moved = pltpu.roll(rows, 0, 1, stride=1, stride_axis=0)
            out[comp, kind] = moved.T.astype(jnp.bfloat16)


def banded(kernels):
    comps, kinds, width = kernels.shape
    return pl.pallas_call(
        bands_kernel,
        out_shape=jax.ShapeDtypeStruct((comps, kinds, 2 * width, width), kernels.dtype),
        in_specs=[vmem()],
        out_specs=vmem(),
        compiler_params=pltpu.CompilerParams(vmem_limit_bytes=FIRST_LIMIT),
        name="banded",
    )(kernels)


def chunk(scalars, slots, tables, carried, residues, first, last):
    own = slots[0][2]
    segs, step, comps, sub, cols = own.shape
    ranks = step
    rows = ranks * sub
    size = step * rows
    mats, bands = tables
    kinds = bands.shape[1]
    count = cols // BLOCK
    outs = [] if first else [(-1, residues[0] - 1)]
    outs += [(block, residues[0] + block) for block in range(count - 1)]
    if last:
        outs.append((count - 1, residues[-1]))
    window = rows + SUB
    tall = size + rows
    edge = jax.ShapeDtypeStruct((segs, comps, tall, BLOCK), jnp.bfloat16)
    total = jax.ShapeDtypeStruct((kinds, ranks, rows, BLOCK), jnp.float32)
    flat = (kinds // 2 * ranks * rows, BLOCK)
    if last:
        out_shape = [
            jax.ShapeDtypeStruct(flat, jnp.float32),
            jax.ShapeDtypeStruct(flat, jnp.bfloat16),
        ]
    else:
        out_shape = [total, edge]
    if first:
        out_shape.append(edge)
    pieces = tuple((slot[0], slot[1], len(slot) - 2) for slot in slots)
    plan = (pieces, first, last, tuple(outs), segs, kinds)
    arrays = [array for slot in slots for array in slot[2:]]
    inputs = [*scalars, *arrays, mats, bands, *carried]
    specs = [smem()] * 2 + [vmem()] * (len(inputs) - 2)
    scratch = [
        pltpu.VMEM((segs, step, comps, ranks, sub, cols), jnp.bfloat16),
        pltpu.VMEM((step, comps * rows, 2 * BLOCK), jnp.float32),
        pltpu.VMEM((count, segs, comps, tall, BLOCK), jnp.bfloat16),
        pltpu.VMEM((2, segs * len(outs), window, BLOCK), jnp.float32),
    ]
    if last:
        scratch.append(pltpu.VMEM(total.shape, total.dtype))
    return pl.pallas_call(
        functools.partial(chunk_kernel, plan),
        out_shape=out_shape,
        in_specs=specs,
        out_specs=[vmem()] * len(out_shape),
        scratch_shapes=scratch,
        compiler_params=pltpu.CompilerParams(vmem_limit_bytes=CHUNK_LIMIT),
        cost_estimate=pl.CostEstimate(
            flops=2 * segs * len(outs) * kinds * window * 4 * BLOCK * 2 * BLOCK
            + 8 * segs * step * rows * rows * cols,
            bytes_accessed=8 * total.size,
            transcendentals=0,
        ),
        name="chunk",
    )(*inputs)


def line_body(samples, kernels, offsets, weight_index, level_weights):
    segs, _, rows, cols_two = samples.shape
    ranks = lax.axis_size("freq")
    size_one = rows * ranks
    length = size_one * cols_two
    kinds = kernels.shape[1]
    blocks_here = length // ranks // BLOCK
    places = jnp.stack([lax.axis_index("freq"), lax.axis_index("seg")]).astype(jnp.int32)
    groups = np.split(np.arange(ranks), SPLITS)
    heights, tables = first_tables(samples, ranks)
    tables = jnp.asarray(tables)
    turned = []
    for group in groups:
        turned.append(
            first_stage(
                samples, heights, tables, ranks, group[0] * BLOCK, group.size * BLOCK
            )
        )

    times_of = np.arange(ranks)[:, None, None] + ranks * np.arange(rows)[None, None, :]
    real, imag = phases(times_of * np.arange(rows)[None, :, None], size_one)
    mats = np.concatenate(
        [np.concatenate([real, -imag], 2), np.concatenate([imag, real], 2)], 1
    ).astype(jnp.bfloat16)
    bands = banded(kernels)

    slots = []
    for own in turned:
        slots.append(gathered(own))

    bins = jnp.remainder(
        lax.axis_index("freq") * blocks_here + offsets.reshape(segs * kinds), ranks * blocks_here
    )
    row = bins // ranks
    lane = bins - row * ranks
    row_start = row // SUB * SUB
    ints = jnp.concatenate([places, row_start, row - row_start, lane])
    levels = lax.broadcasted_iota(jnp.int32, (segs, level_weights.shape[0]), 1)
    weights = jnp.sum(jnp.where(weight_index[:, None] == levels, level_weights[None, :], 0.0), 1)
    weights = weights * (1.0 / (segs * lax.axis_size("seg")))
    scalars = (ints, weights)

    carried = []
    rolled = None
    for number, group in enumerate(groups):
        first = number == 0
        last = number == len(groups) - 1
        if last:
            carried = carried + [rolled]
        result = chunk(
            scalars, slots[number], (mats, bands), carried, list(group), first, last
        )
        if first:
            rolled = result[2]
        carried = [result[1], result[0]]
    send, own = carried
    other = lax.ppermute(send, "seg", [(i, 1 - i) for i in range(2)])
    out = own + other.astype(jnp.float32)
    owned = kinds // 2
    out = jnp.swapaxes(out.reshape(blocks_here, owned, BLOCK), 0, 1)
    return out.reshape(owned, blocks_here * BLOCK)


def solution(mesh):
    in_specs = (
        P(("parts", "seg"), None, "freq", None),
        P(),
        P(("parts", "seg"), None),
        P(("parts", "seg")),
        P(),
    )
    out_specs = P(("parts", "seg"), "freq")
    line = mesh.shape["freq"] == LINE * PAIR and mesh.shape["seg"] == 2

    def body(samples, *others):
        if not line:
            return spread_body(samples, *others)
        return line_body(samples, *others)

    return jax.shard_map(body, mesh=mesh, in_specs=in_specs, out_specs=out_specs, check_vma=False)
```

```python
import functools
import math

import jax
import jax.numpy as jnp
import numpy as np
from jax import lax
from jax.experimental import pallas as pl
from jax.experimental.pallas import tpu as pltpu
from jax.sharding import PartitionSpec as P


BLOCK = 128
KERNELS = 8
REACH = 4
ROUTE_CAP = 4
SPLITS = (4,)
FIRST_LIMIT = 60 * 2**20
CHUNK_LIMIT = 34 * 2**20


def extended(cells, sides, width):
    for axis, dim in sides:
        count = lax.axis_size(axis)
        head = lax.slice_in_dim(cells, 0, width, axis=dim)
        tail = lax.slice_in_dim(cells, cells.shape[dim] - width, cells.shape[dim], axis=dim)
        cells = jnp.concatenate(
            [
                lax.ppermute(tail, axis, [(i, (i + 1) % count) for i in range(count)]),
                cells,
                lax.ppermute(head, axis, [((i + 1) % count, i) for i in range(count)]),
            ],
            axis=dim,
        )
    return cells


def passed_along(block, axis, distance):
    devices = range(lax.axis_size(axis))
    route = [((i - distance) % len(devices), i) for i in devices]
    return lax.ppermute(block, axis, route)


def dft_table(size):
    rows = lax.broadcasted_iota(jnp.int32, (size, size), 0)
    cols = lax.broadcasted_iota(jnp.int32, (size, size), 1)
    angle = (rows * cols % size).astype(jnp.float32) * (2.0 * math.pi / size)
    return (jnp.cos(angle), jnp.sin(angle))


def toeplitz(kernels):
    width = kernels.shape[-1]
    tail = jnp.zeros(kernels.shape[:-1] + (width + 1,), kernels.dtype)
    padded = jnp.concatenate([kernels, tail], -1)
    tiled = jnp.tile(padded, (1, 1, width))[..., : 2 * width * width]
    return tiled.reshape(kernels.shape[:-1] + (width, 2 * width))


def take_blocks(joined, start):
    return lax.dynamic_slice_in_dim(joined, start, joined.shape[0] // 2, 0)


def slide(joined, starts):
    return jax.vmap(jax.vmap(take_blocks))(joined, starts)


def spread_body(samples, kernels, offsets, weight_index, level_weights):
    segs, comps, rows_one, cols_two = samples.shape
    ranks = lax.axis_size("freq")
    here = lax.axis_index("freq")
    size_one = rows_one * ranks
    length = size_one * cols_two
    highest = lax.Precision.HIGHEST
    cos_two, sin_two = dft_table(cols_two)
    stacked = samples.reshape(segs * comps * rows_one, cols_two)
    with_cos = jnp.dot(stacked, cos_two, precision=highest).reshape(samples.shape)
    with_sin = jnp.dot(stacked, sin_two, precision=highest).reshape(samples.shape)
    first_real = with_cos[:, 0] + with_sin[:, 1]
    first_imag = with_cos[:, 1] - with_sin[:, 0]
    row_global = here * rows_one + lax.broadcasted_iota(jnp.int32, (rows_one, cols_two), 0)
    col_global = lax.broadcasted_iota(jnp.int32, (rows_one, cols_two), 1)
    twist = (row_global * col_global % length).astype(jnp.float32) * (2.0 * math.pi / length)
    twist_cos = jnp.cos(twist)
    twist_sin = jnp.sin(twist)
    turned = jnp.stack(
        [
            first_real * twist_cos + first_imag * twist_sin,
            first_imag * twist_cos - first_real * twist_sin,
        ],
        1,
    )
    columns = lax.all_to_all(
        turned.astype(jnp.bfloat16), "freq", split_axis=3, concat_axis=3, tiled=True
    ).astype(turned.dtype)
    width_two = cols_two // ranks
    ordered = columns.reshape(segs, comps, rows_one, ranks, width_two)
    cos_one, sin_one = dft_table(size_one)
    cos_one = cos_one.reshape(ranks, rows_one, size_one)
    sin_one = sin_one.reshape(ranks, rows_one, size_one)
    second_cos = jnp.einsum("scirl,rik->sclk", ordered, cos_one, precision=highest)
    second_sin = jnp.einsum("scirl,rik->sclk", ordered, sin_one, precision=highest)
    second = jnp.stack(
        [second_cos[:, 0] + second_sin[:, 1], second_cos[:, 1] - second_sin[:, 0]], 1
    )
    arrived = lax.all_to_all(
        second.astype(jnp.bfloat16), "freq", split_axis=3, concat_axis=3, tiled=True
    ).astype(second.dtype)
    width_one = size_one // ranks
    spectrum = arrived.reshape(segs, comps, width_two, ranks, width_one)
    spectrum = jnp.transpose(spectrum, (0, 1, 4, 3, 2)).reshape(segs, comps, width_one * cols_two)
    spectrum = (spectrum * (1.0 / math.sqrt(length))).astype(jnp.bfloat16)
    half = BLOCK // 2
    edged = extended(spectrum, (("freq", 2),), half)
    bins_here = spectrum.shape[2]
    count = bins_here // BLOCK
    lower = edged[..., :bins_here].reshape(segs, comps, count, BLOCK)
    upper = edged[..., BLOCK:].reshape(segs, comps, count, BLOCK)
    window = jnp.concatenate([lower, upper], -1)
    bands = toeplitz(kernels)
    real_band = bands[0]
    imag_band = bands[1]
    table = jnp.stack(
        [jnp.stack([real_band, imag_band], 0), jnp.stack([-imag_band, real_band], 0)], 0
    )
    filtered = jnp.einsum("scbm,cokim->skboi", window, table, preferred_element_type=jnp.float32)
    power = (filtered[:, :, :, 0] ** 2 + filtered[:, :, :, 1] ** 2).astype(jnp.bfloat16)
    quotient = jnp.floor_divide(offsets, count)
    remainder = offsets - quotient * count
    following = passed_along(power, "freq", -1)
    inner = slide(jnp.concatenate([power, following], 2), remainder)
    plane_count = segs * KERNELS
    flat = inner.reshape(plane_count, count * BLOCK)
    plane_quot = quotient.reshape(plane_count)
    distances = lax.broadcasted_iota(jnp.int32, (2 * REACH + 1, plane_count), 0) - REACH
    member = (plane_quot[None, :] == distances).astype(jnp.int32)
    place = jnp.cumsum(member, 1) - 1
    slot_ids = lax.broadcasted_iota(jnp.int32, (2 * REACH + 1, ROUTE_CAP, plane_count), 1)
    select = ((member[:, None, :] == 1) & (place[:, None, :] == slot_ids)).astype(jnp.bfloat16)
    packed = jnp.einsum("dcp,pl->dcl", select, flat, preferred_element_type=jnp.float32).astype(
        jnp.bfloat16
    )
    received = []
    for step_index in range(2 * REACH + 1):
        received.append(passed_along(packed[step_index], "freq", -(step_index - REACH)))
    gathered = jnp.stack(received, 0)
    placed = jnp.einsum("dcp,dcl->pl", select, gathered, preferred_element_type=jnp.float32)
    shifted = placed.astype(jnp.bfloat16).reshape(segs, KERNELS, count, BLOCK)
    levels = lax.broadcasted_iota(jnp.int32, (segs, level_weights.shape[0]), 1)
    weights = jnp.sum(jnp.where(weight_index[:, None] == levels, level_weights[None, :], 0.0), 1)
    scale = 1.0 / (segs * lax.axis_size("seg"))
    partial_sum = jnp.sum((weights * scale)[:, None, None, None] * shifted.astype(jnp.float32), 0)
    owned = lax.psum_scatter(
        partial_sum.astype(jnp.bfloat16), "seg", scatter_dimension=0, tiled=True
    ).astype(jnp.float32)
    return owned.reshape(owned.shape[0], count * BLOCK)


LINE = 4
PAIR = 2
SUB = 16
GROUP = 32


def phases(products, size):
    angle = (np.asarray(products, np.int64) % size) * (2.0 * math.pi / size)
    return np.cos(angle).astype(np.float32), (-np.sin(angle)).astype(np.float32)


def times(a, b):
    return a[0] * b[0] - a[1] * b[1], a[0] * b[1] + a[1] * b[0]


def vmem():
    return pl.BlockSpec(memory_space=pltpu.VMEM)


def smem():
    return pl.BlockSpec(memory_space=pltpu.SMEM)


def first_kernel(begin, heights, x_hbm, tables_hbm, out, x, tables, er, ei, wr, wi, sems):
    segs, comps, rows, length = x.shape
    step, sub, cols = out.shape[1], out.shape[3], out.shape[4]
    copies = [
        pltpu.make_async_copy(tables_hbm.at[:, pl.ds(begin, cols)], tables, sems.at[segs])
    ]
    for seg in range(segs):
        copies.append(pltpu.make_async_copy(x_hbm.at[seg], x.at[seg], sems.at[seg]))
    for copy in copies:
        copy.start()
    here = lax.axis_index("freq")
    at = np.concatenate([[0], np.cumsum(heights)])

    def table(number, row=0, height=None):
        height = heights[number] if height is None else height
        return tables[pl.ds(int(at[number]) + row, height), :]

    fine = heights[2]
    copies[0].wait()
    inner = (table(2), table(3))
    for coarse in range(heights[0]):
        real, imag = times((table(0, coarse, 1), table(1, coarse, 1)), inner)
        er[pl.ds(coarse * fine, fine), :] = real.astype(jnp.bfloat16)
        ei[pl.ds(coarse * fine, fine), :] = imag.astype(jnp.bfloat16)
    for seg in range(segs):
        copies[1 + seg].wait()
        series = x[seg].astype(jnp.bfloat16).reshape(comps * rows, length)
        for phase, kept in ((er, wr), (ei, wi)):
            value = jnp.dot(series, phase[...], preferred_element_type=jnp.float32)
            for block in range(kept.shape[1]):
                kept[seg, block] = value[:, block * BLOCK : (block + 1) * BLOCK]
        for block in range(wr.shape[1]):
            lanes = slice(block * BLOCK, (block + 1) * BLOCK)
            turned = (table(6)[:, lanes], table(7)[:, lanes])
            for turn in range(step):
                row = here * step + turn
                twist = times((table(4, row, 1)[:, lanes], table(5, row, 1)[:, lanes]), turned)
                low = pl.ds(turn, sub, stride=step)
                high = pl.ds(rows + turn, sub, stride=step)
                value = (
                    wr[seg, block, low, :] - wi[seg, block, high, :],
                    wi[seg, block, low, :] + wr[seg, block, high, :],
                )
                real, imag = times(value, twist)
                out[seg, turn, 0, :, lanes] = real.astype(jnp.bfloat16)
                out[seg, turn, 1, :, lanes] = imag.astype(jnp.bfloat16)


def first_tables(samples, ranks):
    _, _, rows, length = samples.shape
    columns = np.arange(length) - BLOCK // 2
    size = rows * ranks * length
    scale = np.float32(1.0 / math.sqrt(size))
    coarse = phases(np.arange(length // GROUP)[:, None] * GROUP * columns[None], length)
    fine = phases(np.arange(GROUP)[:, None] * columns[None], length)
    outer = np.arange(ranks)[:, None] * rows + np.arange(ranks)[None]
    outer = [scale * part for part in phases(outer.reshape(-1, 1) * columns[None], size)]
    inner = phases(np.arange(rows // ranks)[:, None] * ranks * columns[None], size)
    parts = [*coarse, *fine, *outer, *inner]
    return tuple(part.shape[0] for part in parts), np.concatenate(parts, 0)


def first_stage(samples, heights, tables, ranks, begin, cols):
    segs, comps, rows, length = samples.shape
    sub = rows // ranks
    return pl.pallas_call(
        functools.partial(first_kernel, begin, heights),
        out_shape=jax.ShapeDtypeStruct((segs, ranks, comps, sub, cols), jnp.bfloat16),
        in_specs=[pl.BlockSpec(memory_space=pl.ANY)] * 2,
        out_specs=vmem(),
        scratch_shapes=[
            pltpu.VMEM(samples.shape, samples.dtype),
            pltpu.VMEM((tables.shape[0], cols), tables.dtype),
        ]
        + [pltpu.VMEM((length, cols), jnp.bfloat16)] * 2
        + [pltpu.VMEM((segs, cols // BLOCK, comps * rows, BLOCK), jnp.float32)] * 2
        + [pltpu.SemaphoreType.DMA((segs + 1,))],
        compiler_params=pltpu.CompilerParams(vmem_limit_bytes=FIRST_LIMIT),
        cost_estimate=pl.CostEstimate(
            flops=2 * segs * comps * rows * length * 2 * cols,
            bytes_accessed=4 * samples.size,
            transcendentals=0,
        ),
        name="first_stage",
    )(samples, tables)


def gathered(own, number):
    near = [(i, i ^ PAIR) for i in range(PAIR * LINE)]
    far = [(i, i ^ (2 * PAIR)) for i in range(PAIR * LINE)]
    flip = [(i, i ^ 1) for i in range(PAIR * LINE)]
    middle = [(i, i ^ (3 * PAIR)) for i in range(PAIR, 3 * PAIR)]
    ends = [(i, i ^ PAIR) for i in range(PAIR, 3 * PAIR)]

    def send(array, route):
        return lax.ppermute(array, "freq", route)

    by_near = send(own, near)
    crossed = send(own, middle)
    by_flip = send(own, flip)
    by_far = send(own, far)
    if number % 2:
        near_flip = send(by_flip, near)
    else:
        near_flip = send(by_near, flip)
    far_flip = send(by_far, flip)
    relayed = send(by_far, ends)
    flip_middle = send(crossed, [pair for pair in flip if pair[0] in dict(middle)])
    flip_ends = send(relayed, [pair for pair in flip if pair[0] not in dict(middle)])
    return [
        (0, 0, own),
        (1, 0, by_flip),
        (PAIR, 0, by_near),
        (PAIR + 1, 0, near_flip),
        (2 * PAIR, 0, by_far),
        (2 * PAIR + 1, 0, far_flip),
        (3 * PAIR, 0, crossed, relayed),
        (3 * PAIR + 1, 0, flip_middle, flip_ends),
    ]


def eight(z):
    root = np.float32(math.sqrt(0.5))

    def add(a, b):
        return a[0] + b[0], a[1] + b[1]

    def sub(a, b):
        return a[0] - b[0], a[1] - b[1]

    def four(a, b, c, d):
        p, q, r, s = add(a, c), sub(a, c), add(b, d), sub(b, d)
        return (
            add(p, r),
            (q[0] + s[1], q[1] - s[0]),
            sub(p, r),
            (q[0] - s[1], q[1] + s[0]),
        )

    even = four(z[0], z[2], z[4], z[6])
    odd = list(four(z[1], z[3], z[5], z[7]))
    x, y = odd[1]
    odd[1] = ((x + y) * root, (y - x) * root)
    x, y = odd[2]
    odd[2] = (y, -x)
    x, y = odd[3]
    odd[3] = ((y - x) * root, -(x + y) * root)
    return [add(even[m], odd[m]) for m in range(4)] + [sub(even[m], odd[m]) for m in range(4)]


def chunk_kernel(plan, *refs):
    pieces, first, last, outs, segs, kinds = plan
    planes = segs * kinds
    refs = list(refs)
    ints, weight = refs.pop(0), refs.pop(0)
    slots = [[refs.pop(0) for _ in range(many)] for _, _, many in pieces]
    mats, bands = refs.pop(0), refs.pop(0)
    before = None if first else refs.pop(0)
    total_in = None if first else refs.pop(0)
    after = refs.pop(0) if last else None
    if last:
        mine_out, send_out = refs.pop(0), refs.pop(0)
    else:
        total, edge_out = refs.pop(0), refs.pop(0)
    if first:
        after = refs.pop(0)
    parts, mixed, held, power = (refs.pop(0) for _ in range(4))
    if last:
        total = refs.pop(0)

    def row_start(plane):
        return ints[2 + plane]

    def row_shift(plane):
        return ints[2 + planes + plane]

    def lane_start(plane):
        return ints[2 + 2 * planes + plane]

    for (distance, start, _), arrays in zip(pieces, slots):
        place = lax.bitwise_xor(ints[0], distance)
        for seg in range(arrays[0].shape[0]):
            for turn in range(parts.shape[1]):
                for comp in range(parts.shape[2]):
                    value = arrays[0][seg, turn, comp]
                    for other in arrays[1:]:
                        value = value + other[seg, turn, comp]
                    parts[start + seg, turn, comp, place] = value
    _, step, comps, ranks, sub, cols = parts.shape
    rows = ranks * sub
    count = cols // BLOCK
    size = step * rows
    wrap = held.shape[3] - size
    for seg in range(segs):
        for low in range(0, cols, 2 * BLOCK):
            width = min(2 * BLOCK, cols - low)
            for turn in range(step):
                value = parts[seg, turn, :, :, :, low : low + width]
                mixed[turn, :, :width] = jnp.dot(
                    mats[turn],
                    value.reshape(comps * rows, width),
                    preferred_element_type=jnp.float32,
                )
            for lane in range(0, width, BLOCK):
                block = (low + lane) // BLOCK
                lanes = slice(lane, lane + BLOCK)
                for row in range(0, rows, SUB):
                    z = [
                        (
                            mixed[turn, row : row + SUB, lanes],
                            mixed[turn, rows + row : rows + row + SUB, lanes],
                        )
                        for turn in range(step)
                    ]
                    for turn, value in enumerate(eight(z)):
                        for comp in range(2):
                            one = value[comp].astype(jnp.bfloat16)
                            at = turn * rows + row
                            held[block, seg, comp, at : at + SUB, :] = one
                            if at < wrap:
                                held[block, seg, comp, size + at : size + at + SUB, :] = one
    if not last:
        edge_out[...] = held[count - 1]
    if first:
        for seg in range(segs):
            for comp in range(comps):
                value = held[0, seg, comp, :, :].astype(jnp.float32)
                value = pltpu.roll(value, value.shape[0] - 1, 0).astype(jnp.bfloat16)
                after[seg, comp, :size, :] = value[:size]
                after[seg, comp, size:, :] = value[:wrap]
        total[...] = jnp.zeros_like(total)
    else:
        total[...] = total_in[...]

    def row_block(block, seg, comp, at):
        if block < 0:
            return before[seg, comp, at, :]
        if block == count:
            return after[seg, comp, at, :]
        return held[block, seg, comp, at, :]

    window = power.shape[2]
    for kind in range(kinds):
        real_band, imag_band = bands[0, kind], bands[1, kind]
        table = (
            jnp.concatenate([real_band, imag_band], 1),
            jnp.concatenate([-imag_band, real_band], 1),
        )
        lines = []
        for seg in range(segs):
            at = pl.ds(pl.multiple_of(row_start(seg * kinds + kind), SUB), window)
            for block, _ in outs:
                lines.append(
                    jnp.concatenate(
                        [
                            row_block(block + side, seg, comp, at)
                            for comp in range(2)
                            for side in range(2)
                        ],
                        1,
                    )
                )
        value = jnp.dot(
            jnp.concatenate(lines, 0),
            jnp.concatenate(table, 0),
            preferred_element_type=jnp.float32,
        )
        value = value[:, :BLOCK] ** 2 + value[:, BLOCK:] ** 2
        number = 0
        for seg in range(segs):
            plane = seg * kinds + kind
            lane = lane_start(plane)
            for _, residue in outs:
                power[kind % 2, number] = value[number * window : (number + 1) * window]
                carry = jnp.where(residue < lane, 1, 0)
                place = residue - lane + carry * ranks
                moved = power[kind % 2, number, pl.ds(row_shift(plane) + carry, rows), :]
                total[kind, place] = total[kind, place] + weight[seg] * moved
                number += 1
    if last:
        owned = kinds // 2
        theirs_at = owned * (1 - ints[1])
        mine_at = owned * ints[1]
        lane_rows = 8
        for target, base in ((send_out, theirs_at), (mine_out, mine_at)):
            for row in range(0, rows, lane_rows):
                tiles = [
                    total[base + kind, place, row : row + lane_rows, :]
                    for place in range(ranks)
                    for kind in range(owned)
                ]
                value = jnp.swapaxes(jnp.stack(tiles, 0), 0, 1).reshape(-1, BLOCK)
                height = value.shape[0]
                at = row // lane_rows * height
                target[at : at + height, :] = value.astype(target.dtype)


def bands_kernel(kernels, out):
    comps, kinds, width = kernels.shape
    for comp in range(comps):
        for kind in range(kinds):
            row = kernels[comp, kind : kind + 1, :].astype(jnp.float32)
            rows = jnp.broadcast_to(jnp.concatenate([row, jnp.zeros_like(row)], 1), (width, 2 * width))
            moved = pltpu.roll(rows, 0, 1, stride=1, stride_axis=0)
            out[comp, kind] = moved.T.astype(jnp.bfloat16)


def banded(kernels):
    comps, kinds, width = kernels.shape
    return pl.pallas_call(
        bands_kernel,
        out_shape=jax.ShapeDtypeStruct((comps, kinds, 2 * width, width), kernels.dtype),
        in_specs=[vmem()],
        out_specs=vmem(),
        compiler_params=pltpu.CompilerParams(vmem_limit_bytes=FIRST_LIMIT),
        name="banded",
    )(kernels)


def chunk(scalars, slots, tables, carried, residues, first, last):
    own = slots[0][2]
    segs, step, comps, sub, cols = own.shape
    ranks = step
    rows = ranks * sub
    size = step * rows
    mats, bands = tables
    kinds = bands.shape[1]
    count = cols // BLOCK
    outs = [] if first else [(-1, residues[0] - 1)]
    outs += [(block, residues[0] + block) for block in range(count - 1)]
    if last:
        outs.append((count - 1, residues[-1]))
    window = rows + SUB
    tall = size + rows
    edge = jax.ShapeDtypeStruct((segs, comps, tall, BLOCK), jnp.bfloat16)
    total = jax.ShapeDtypeStruct((kinds, ranks, rows, BLOCK), jnp.float32)
    flat = (kinds // 2 * ranks * rows, BLOCK)
    if last:
        out_shape = [
            jax.ShapeDtypeStruct(flat, jnp.float32),
            jax.ShapeDtypeStruct(flat, jnp.bfloat16),
        ]
    else:
        out_shape = [total, edge]
    if first:
        out_shape.append(edge)
    pieces = tuple((slot[0], slot[1], len(slot) - 2) for slot in slots)
    plan = (pieces, first, last, tuple(outs), segs, kinds)
    arrays = [array for slot in slots for array in slot[2:]]
    inputs = [*scalars, *arrays, mats, bands, *carried]
    specs = [smem()] * 2 + [vmem()] * (len(inputs) - 2)
    scratch = [
        pltpu.VMEM((segs, step, comps, ranks, sub, cols), jnp.bfloat16),
        pltpu.VMEM((step, comps * rows, 2 * BLOCK), jnp.float32),
        pltpu.VMEM((count, segs, comps, tall, BLOCK), jnp.bfloat16),
        pltpu.VMEM((2, segs * len(outs), window, BLOCK), jnp.float32),
    ]
    if last:
        scratch.append(pltpu.VMEM(total.shape, total.dtype))
    return pl.pallas_call(
        functools.partial(chunk_kernel, plan),
        out_shape=out_shape,
        in_specs=specs,
        out_specs=[vmem()] * len(out_shape),
        scratch_shapes=scratch,
        compiler_params=pltpu.CompilerParams(vmem_limit_bytes=CHUNK_LIMIT),
        cost_estimate=pl.CostEstimate(
            flops=2 * segs * len(outs) * kinds * window * 4 * BLOCK * 2 * BLOCK
            + 8 * segs * step * rows * rows * cols,
            bytes_accessed=8 * total.size,
            transcendentals=0,
        ),
        name="chunk",
    )(*inputs)


def line_body(samples, kernels, offsets, weight_index, level_weights):
    segs, _, rows, cols_two = samples.shape
    ranks = lax.axis_size("freq")
    size_one = rows * ranks
    length = size_one * cols_two
    kinds = kernels.shape[1]
    blocks_here = length // ranks // BLOCK
    places = jnp.stack([lax.axis_index("freq"), lax.axis_index("seg")]).astype(jnp.int32)
    groups = np.split(np.arange(ranks), SPLITS)
    heights, tables = first_tables(samples, ranks)
    tables = jnp.asarray(tables)
    turned = []
    for group in groups:
        turned.append(
            first_stage(
                samples, heights, tables, ranks, group[0] * BLOCK, group.size * BLOCK
            )
        )

    times_of = np.arange(ranks)[:, None, None] + ranks * np.arange(rows)[None, None, :]
    real, imag = phases(times_of * np.arange(rows)[None, :, None], size_one)
    mats = np.concatenate(
        [np.concatenate([real, -imag], 2), np.concatenate([imag, real], 2)], 1
    ).astype(jnp.bfloat16)
    bands = banded(kernels)

    slots = []
    for number, own in enumerate(turned):
        slots.append(gathered(own, number))

    bins = jnp.remainder(
        lax.axis_index("freq") * blocks_here + offsets.reshape(segs * kinds), ranks * blocks_here
    )
    row = bins // ranks
    lane = bins - row * ranks
    row_start = row // SUB * SUB
    ints = jnp.concatenate([places, row_start, row - row_start, lane])
    levels = lax.broadcasted_iota(jnp.int32, (segs, level_weights.shape[0]), 1)
    weights = jnp.sum(jnp.where(weight_index[:, None] == levels, level_weights[None, :], 0.0), 1)
    weights = weights * (1.0 / (segs * lax.axis_size("seg")))
    scalars = (ints, weights)

    carried = []
    rolled = None
    for number, group in enumerate(groups):
        first = number == 0
        last = number == len(groups) - 1
        if last:
            carried = carried + [rolled]
        result = chunk(
            scalars, slots[number], (mats, bands), carried, list(group), first, last
        )
        if first:
            rolled = result[2]
        carried = [result[1], result[0]]
    send, own = carried
    other = lax.ppermute(send, "seg", [(i, 1 - i) for i in range(2)])
    out = own + other.astype(jnp.float32)
    owned = kinds // 2
    out = jnp.swapaxes(out.reshape(blocks_here, owned, BLOCK), 0, 1)
    return out.reshape(owned, blocks_here * BLOCK)


def solution(mesh):
    in_specs = (
        P(("parts", "seg"), None, "freq", None),
        P(),
        P(("parts", "seg"), None),
        P(("parts", "seg")),
        P(),
    )
    out_specs = P(("parts", "seg"), "freq")
    line = mesh.shape["freq"] == LINE * PAIR and mesh.shape["seg"] == 2

    def body(samples, *others):
        if not line:
            return spread_body(samples, *others)
        return line_body(samples, *others)

    return jax.shard_map(body, mesh=mesh, in_specs=in_specs, out_specs=out_specs, check_vma=False)
```
